128 devices in a mesh: pts: 64 (over z, x, y), grp: 2 (over core).
Axes of the slice: x: 4, y: 4, z: 4, core: 2. Of those that a mesh axis runs over, the one named last changes fastest.
Arguments:
- cam_jac: float32 [18, 1048576], P(None, ('pts', 'grp')), may hold values from -0.25 to 0.25
- pt_jac: float32 [6, 1048576], P(None, ('pts', 'grp')), may hold values from -6 to 6
- resid: float32 [2, 1048576], P(None, ('pts', 'grp')), may hold values from -102 to 102
- obs_point: int32 [1048576], P(('pts', 'grp')), may hold values from 0 to 262143, as said below
- obs_camera: int32 [1048576], P(('pts', 'grp')), may hold values from 0 to 2047
- camera_slot: int32 [2048], replicated, may hold values from 0 to 2047, each once
Outputs:
- cam_inverse: float32 [81, 2048], P(None, ('pts', 'grp'))
- precond: float32 [9, 1048576], P(None, ('pts', 'grp'))
The draws below stay inside these ranges and needn't reach their ends.
Inputs may be any that keep to these rules, and one draw needn't show every extreme that they name: `obs_point`: observation o names a point of block o // 8192, from (o // 8192) * 2048 to (o // 8192 + 1) * 2048 - 1; within each block of 8192 observations the point number never falls and rises by at most 1 from one observation to the next, and the block's first observation names the block's first point. Each slot appears once; camera c is owned by device camera_slot[c] // 16 of the joined axes pts+grp.
All inputs are finite; a program needn't handle non-finite values.
Results may differ from the reference program's by a relative error of at most 0.0003.
Values sent between devices are 32-bit elements; how exact they have to be, the bound alone decides.
A program may use at most 64 MiB of HBM per device.

```python
import math
import jax
import jax.numpy as jnp
import numpy as np
from jax import lax

OBS_DEV = 8192
CAM_DEV = 16
PTS_DEV = 2048
OBS = 1048576
CAMS = 2048
N_PTS = 64
N_GRP = 2


def draw_obs_point(key, part):
    devices = OBS // OBS_DEV
    coins = jax.random.randint(jax.random.fold_in(key, 17), (devices, OBS_DEV), 0, 3, dtype=jnp.int32)
    rises = (coins == 0).astype(jnp.int32)
    rises = rises.at[:, 0].set(0)
    local = jnp.minimum(jnp.cumsum(rises, axis=1), PTS_DEV - 1).astype(jnp.int32)
    owner = jnp.arange(devices, dtype=jnp.int32)[:, None] * PTS_DEV
    return (owner + local).reshape(OBS).astype(jnp.int32)


def set_ends(values, rng, low, top_value):
    place = [jax.random.randint(jax.random.fold_in(rng, axis), (), 0, length) for axis, length in enumerate(values.shape)]
    longest = values.shape.index(max(values.shape))
    beside = place[:longest] + [(place[longest] + 1) % values.shape[longest]] + place[longest + 1:]
    return values.at[tuple(place)].set(low).at[tuple(beside)].set(top_value)


def levels(stream_key, dims, shards, smallest, high):
    level, own = 1.0, jax.random.fold_in(stream_key, 6)
    for dim, parts in shards:
        steps = jnp.exp(jax.random.uniform(jax.random.fold_in(own, dim), (parts,), jnp.float32, smallest / len(shards), high / len(shards)))
        level = level * jnp.repeat(steps, dims[dim] // parts).reshape([-1 if axis == dim else 1 for axis in range(len(dims))])
    return level


def cumulative_ranks(amount, skew):
    weights = [(1 << 20) // math.isqrt(standing ** skew) + 1 for standing in range(1, amount + 1)]
    width = 1 + sum(weights) // (1 << 30)
    return np.cumsum(np.array([max(1, weight // width) for weight in weights]))


def ranked_ids(stream_key, shape, amount, lean):
    table = cumulative_ranks(amount, lean)
    ticket = jax.random.randint(jax.random.fold_in(stream_key, 1), shape, 0, int(table[amount - 1]))
    standing = jnp.searchsorted(jnp.asarray(table, jnp.int32), ticket, side="right")
    return jax.random.permutation(jax.random.fold_in(stream_key, 2), amount)[standing].astype(jnp.int32)


def normal_values(stream_key, dims, width, bound, shards=(), kind=jnp.bfloat16):
    drawn = jax.random.normal(stream_key, dims, jnp.float32) * width
    if len(shards) > 0:
        drawn = levels(stream_key, dims, shards, -0.22, 0.18) * drawn
    return jnp.clip(drawn, min=-bound, max=bound).astype(kind)


def setup_inputs(seed: int = 0) -> dict:
    key_of = jax.random.split(jax.random.key(seed), 7)
    return {
        "cam_jac": normal_values(key_of[0], (18, OBS), (OBS_DEV // CAM_DEV) ** -0.5, 0.25, ((1, 128),), jnp.float32),
        "pt_jac": normal_values(key_of[1], (6, OBS), 1.0, 6.0, ((1, 128),), jnp.float32),
        "resid": normal_values(key_of[2], (2, OBS), (OBS_DEV // CAM_DEV // 32 + 1), 102.0, ((1, 128),), jnp.float32),
        "obs_point": draw_obs_point(jax.random.fold_in(key_of[6], 71), 0),
        "obs_camera": set_ends(ranked_ids(key_of[4], (OBS,), CAMS, 1), jax.random.fold_in(key_of[4], 3), 0, CAMS - 1).astype(jnp.int32),
        "camera_slot": jax.random.permutation(key_of[5], CAMS).astype(jnp.int32),
    }


DAMP = 1.0

def lower_pairs():
    return [(row_at, col_at) for row_at in range(9) for col_at in range(row_at + 1)]

def point_table(pt_jac, resid, local_point, npoints):
    entries = []
    for row_at in range(3):
        for col_at in range(row_at, 3):
            entries.append(pt_jac[row_at] * pt_jac[col_at] + pt_jac[3 + row_at] * pt_jac[3 + col_at])
    for row_at in range(3):
        entries.append(pt_jac[row_at] * resid[0] + pt_jac[3 + row_at] * resid[1])
    stacked = jnp.stack(entries, 0)
    sums = jnp.zeros((9, npoints), jnp.float32).at[:, local_point].add(stacked)
    v00 = sums[0] + DAMP
    v01 = sums[1]
    v02 = sums[2]
    v11 = sums[3] + DAMP
    v12 = sums[4]
    v22 = sums[5] + DAMP
    c00 = v11 * v22 - v12 * v12
    c01 = v02 * v12 - v01 * v22
    c02 = v01 * v12 - v02 * v11
    c11 = v00 * v22 - v02 * v02
    c12 = v01 * v02 - v00 * v12
    c22 = v00 * v11 - v01 * v01
    determ = v00 * c00 + v01 * c01 + v02 * c02
    i00 = c00 / determ
    i01 = c01 / determ
    i02 = c02 / determ
    i11 = c11 / determ
    i12 = c12 / determ
    i22 = c22 / determ
    w_zero = i00 * sums[6] + i01 * sums[7] + i02 * sums[8]
    w_one = i01 * sums[6] + i11 * sums[7] + i12 * sums[8]
    w_two = i02 * sums[6] + i12 * sums[7] + i22 * sums[8]
    table = jnp.stack([i00, i01, i02, i11, i12, i22, w_zero, w_one, w_two], 0)
    return table[:, local_point]

def obs_terms(cam_jac, pt_jac, resid, point_rows, pairs):
    i00, i01, i02, i11, i12, i22 = [point_rows[pos] for pos in range(6)]
    weights = [point_rows[6], point_rows[7], point_rows[8]]
    vinv = ((i00, i01, i02), (i01, i11, i12), (i02, i12, i22))
    prow = [[pt_jac[3 * rowp + inner] for inner in range(3)] for rowp in range(2)]
    usage = [[vinv[outer][0] * prow[rowp][0] + vinv[outer][1] * prow[rowp][1] + vinv[outer][2] * prow[rowp][2] for outer in range(3)] for rowp in range(2)]
    proj_zz = prow[0][0] * usage[0][0] + prow[0][1] * usage[0][1] + prow[0][2] * usage[0][2]
    proj_zo = prow[0][0] * usage[1][0] + prow[0][1] * usage[1][1] + prow[0][2] * usage[1][2]
    proj_oo = prow[1][0] * usage[1][0] + prow[1][1] * usage[1][1] + prow[1][2] * usage[1][2]
    keep = ((1.0 - proj_zz, -proj_zo), (-proj_zo, 1.0 - proj_oo))
    shifted = [resid[rowp] - (prow[rowp][0] * weights[0] + prow[rowp][1] * weights[1] + prow[rowp][2] * weights[2]) for rowp in range(2)]
    reduced = jnp.stack([cam_jac[col_at] * shifted[0] + cam_jac[9 + col_at] * shifted[1] for col_at in range(9)], 0)
    mixed = [[keep[rowp][0] * cam_jac[col_at] + keep[rowp][1] * cam_jac[9 + col_at] for col_at in range(9)] for rowp in range(2)]
    terms = jnp.stack([cam_jac[row_at] * mixed[0][col_at] + cam_jac[9 + row_at] * mixed[1][col_at] for row_at, col_at in pairs], 0)
    return (terms, reduced)

def chol_inverse(rows, pairs):
    entry = {pair: rows[pos] for pos, pair in enumerate(pairs)}
    factor = {}
    for col_at in range(9):
        diag = entry[col_at, col_at] + DAMP
        for inner in range(col_at):
            diag = diag - factor[col_at, inner] * factor[col_at, inner]
        root = jnp.sqrt(diag)
        factor[col_at, col_at] = root
        for row_at in range(col_at + 1, 9):
            value = entry[row_at, col_at]
            for inner in range(col_at):
                value = value - factor[row_at, inner] * factor[col_at, inner]
            factor[row_at, col_at] = value / root
    solved = {}
    for col_at in range(9):
        solved[col_at, col_at] = 1.0 / factor[col_at, col_at]
        for row_at in range(col_at + 1, 9):
            value = factor[row_at, col_at] * solved[col_at, col_at]
            for inner in range(col_at + 1, row_at):
                value = value + factor[row_at, inner] * solved[inner, col_at]
            solved[row_at, col_at] = -value / factor[row_at, row_at]
    result = {}
    for row_at in range(9):
        for col_at in range(row_at + 1):
            value = solved[row_at, row_at] * solved[row_at, col_at]
            for inner in range(row_at + 1, 9):
                value = value + solved[inner, row_at] * solved[inner, col_at]
            result[row_at, col_at] = value
            result[col_at, row_at] = value
    return jnp.stack([result[row_at, col_at] for row_at in range(9) for col_at in range(9)], 0)

def apply_inverse(picked, reduced, locate):
    outputs = []
    for row_at in range(9):
        value = picked[locate[row_at, 0]] * reduced[0]
        for col_at in range(1, 9):
            value = value + picked[locate[row_at, col_at]] * reduced[col_at]
        outputs.append(value)
    return jnp.stack(outputs, 0)

def reference(cam_jac, pt_jac, resid, obs_point, obs_camera, camera_slot):
    pairs = lower_pairs()
    devices = N_PTS * N_GRP

    def blocks(array):
        return jnp.moveaxis(array.reshape(array.shape[0], devices, OBS_DEV), 1, 0)
    slot = camera_slot[obs_camera]
    offsets = jnp.arange(devices, dtype=jnp.int32) * PTS_DEV

    def one_block(total, inputs):
        cam_part, pt_part, res_part, point_part, slot_part, offset = inputs
        rows = point_table(pt_part, res_part, point_part - offset, PTS_DEV)
        terms, reduced = obs_terms(cam_part, pt_part, res_part, rows, pairs)
        return (total.at[:, slot_part].add(terms), reduced)
    total, reduced = lax.scan(one_block, jnp.zeros((len(pairs), CAMS), jnp.float32), (blocks(cam_jac), blocks(pt_jac), blocks(resid), obs_point.reshape(devices, OBS_DEV), slot.reshape(devices, OBS_DEV), offsets))
    inverse = chol_inverse(total, pairs)
    locate = {(row_at, col_at): row_at * 9 + col_at for row_at in range(9) for col_at in range(9)}

    def finish(inputs):
        slot_part, reduced_part = inputs
        return apply_inverse(inverse[:, slot_part], reduced_part, locate)
    precond = lax.map(finish, (slot.reshape(devices, OBS_DEV), reduced))
    precond = jnp.moveaxis(precond, 0, 1).reshape(9, OBS)
    return (inverse, precond)
```

```python
import jax
import jax.numpy as jnp
from jax import lax
from jax.experimental import pallas as pl
from jax.experimental.pallas import tpu as pltpu
from jax.sharding import PartitionSpec as P

F32, BF16, I32 = jnp.float32, jnp.bfloat16, jnp.int32
MESH = pl.DeviceIdType.MESH
XS = 40
TS = 56
OS = 24
PAIRS = [(i, j) for i in range(9) for j in range(i + 1)]
CHIPS = 64


def hops(off):
    return sum(min(d, 4 - d) for d in (off // 16, off // 4 % 4, off % 4))


OFFSETS = sorted(range(1, CHIPS), key=lambda off: (-hops(off), off))


def m8(x):
    return pl.multiple_of(x, 8)


def lane_pick(row, idx):
    return jnp.take_along_axis(row, idx, axis=1, mode="promise_in_bounds")


def find_slots(cid_ref, map_ref, slot_ref):
    def step(g, carry):
        cid = cid_ref[pl.ds(m8(g * 8), 8), :]
        lo = cid & 127
        vals = [lane_pick(map_ref[pl.ds(h, 8, stride=0), :], lo) for h in range(16)]
        for b in range(4):
            bit = ((cid >> (7 + b)) & 1) == 1
            vals = [jnp.where(bit, vals[2 * i + 1], vals[2 * i]) for i in range(len(vals) // 2)]
        slot_ref[pl.ds(m8(g * 8), 8), :] = vals[0]
        return carry

    lax.fori_loop(0, 8, step, 0)


def spread_inputs(cam_ref, pt_ref, res_ref, xs):
    for j in range(64):
        at = pl.ds(j * 128, 128)
        xs[j * XS : j * XS + 8, :] = cam_ref[0:8, at]
        xs[j * XS + 8 : j * XS + 16, :] = cam_ref[8:16, at]
        xs[j * XS + 16 : j * XS + 18, :] = cam_ref[16:18, at]
        xs[j * XS + 24 : j * XS + 30, :] = pt_ref[0:6, at]
        xs[j * XS + 32 : j * XS + 34, :] = res_ref[0:2, at]


def point_sums(pid_ref, xs, tot, heads, tails, fix):
    lane = lax.broadcasted_iota(I32, (8, 128), 1)

    def quantity(g, q):
        return xs[pl.ds(g * (8 * XS) + q, 8, stride=XS), :]

    def step(g, carry):
        p = [[quantity(g, 24 + 3 * k + c) for c in range(3)] for k in range(2)]
        e = [quantity(g, 32 + k) for k in range(2)]
        pid = pid_ref[pl.ds(m8(g * 8), 8), :]
        v = [p[0][a] * p[0][c] + p[1][a] * p[1][c] for a in range(3) for c in range(a, 3)]
        v += [p[0][a] * e[0] + p[1][a] * e[1] for a in range(3)]
        end = lane
        for s in range(7):
            k = 1 << s
            same = (pltpu.roll(pid, k, 1) == pid) & (lane >= k)
            v = [x + jnp.where(same, pltpu.roll(x, k, 1), 0.0) for x in v]
            after = (pltpu.roll(pid, 128 - k, 1) == pid) & (lane < 128 - k)
            end = jnp.where(after, pltpu.roll(end, 128 - k, 1), end)
        head = jnp.zeros((8, 128), F32)
        tail = jnp.zeros((8, 128), F32)
        for q in range(9):
            full = lane_pick(v[q], end)
            tot[pl.ds(m8(q * 64 + g * 8), 8), :] = full
            head = jnp.where(lane == q, jnp.broadcast_to(full[:, 0:1], (8, 128)), head)
            tail = jnp.where(lane == q, jnp.broadcast_to(full[:, 127:128], (8, 128)), tail)
        heads[pl.ds(m8(g * 8), 8), :] = head
        tails[pl.ds(m8(g * 8), 8), :] = tail
        return carry

    lax.fori_loop(0, 8, step, 0)

    pid = pid_ref[...]
    first = jnp.broadcast_to(pid[:, 0:1], (64, 128))
    last = jnp.broadcast_to(pid[:, 127:128], (64, 128))
    ends = jnp.where(lax.broadcasted_iota(I32, (64, 128), 1) < 64, first, last).astype(F32)
    across = jnp.transpose(ends)
    r0 = lax.broadcasted_iota(I32, (64, 64), 0)
    r1 = lax.broadcasted_iota(I32, (64, 64), 1)
    from_before = (r1 < r0) & (across[64:128, :] == first[:, 0:64].astype(F32))
    from_after = (r1 > r0) & (across[0:64, :] == last[:, 0:64].astype(F32))

    def total(which, values):
        return lax.dot_general(
            jnp.where(which, 1.0, 0.0),
            values[...],
            (((1,), (0,)), ((), ())),
            precision=lax.Precision.HIGHEST,
            preferred_element_type=F32,
        )

    fix[0:64, :] = total(from_before, tails)
    fix[64:128, :] = total(from_after, heads)


def camera_sums(pid_ref, slot_ref, xs, tot, fix, red, ts, acc):
    def quantity(g, q):
        return xs[pl.ds(g * (8 * XS) + q, 8, stride=XS), :]

    def dot3(a, b):
        return a[0] * b[0] + a[1] * b[1] + a[2] * b[2]

    iota16 = lax.broadcasted_iota(I32, (16, 128), 0).astype(BF16)
    zero = jnp.zeros((16, 128), BF16)
    one = jnp.ones((16, 128), BF16)
    acc[...] = jnp.zeros((1024, 256), F32)

    def step(g, carry):
        at = pl.ds(m8(g * 8), 8)
        pid = pid_ref[at, :]
        pre = fix[at, :]
        post = fix[pl.ds(m8(64 + g * 8), 8), :]
        is_first = pid == jnp.broadcast_to(pid[:, 0:1], (8, 128))
        is_last = pid == jnp.broadcast_to(pid[:, 127:128], (8, 128))
        s = []
        for q in range(9):
            x = tot[pl.ds(m8(q * 64 + g * 8), 8), :]
            x = x + jnp.where(is_first, jnp.broadcast_to(pre[:, q : q + 1], (8, 128)), 0.0)
            x = x + jnp.where(is_last, jnp.broadcast_to(post[:, q : q + 1], (8, 128)), 0.0)
            s.append(x)
        v00, v01, v02, v11, v12, v22 = s[0] + 1.0, s[1], s[2], s[3] + 1.0, s[4], s[5] + 1.0
        c00 = v11 * v22 - v12 * v12
        c01 = v02 * v12 - v01 * v22
        c02 = v01 * v12 - v02 * v11
        c11 = v00 * v22 - v02 * v02
        c12 = v01 * v02 - v00 * v12
        c22 = v00 * v11 - v01 * v01
        inv = 1.0 / (v00 * c00 + v01 * c01 + v02 * c02)
        i00, i01, i02, i11, i12, i22 = [c * inv for c in (c00, c01, c02, c11, c12, c22)]
        vinv = ((i00, i01, i02), (i01, i11, i12), (i02, i12, i22))
        w = [dot3(vinv[a], s[6:9]) for a in range(3)]
        p = [[quantity(g, 24 + 3 * k + c) for c in range(3)] for k in range(2)]
        e = [quantity(g, 32 + k) for k in range(2)]
        use = [[dot3(vinv[a], p[k]) for a in range(3)] for k in range(2)]
        k00 = 1.0 - dot3(p[0], use[0])
        k01 = -dot3(p[0], use[1])
        k11 = 1.0 - dot3(p[1], use[1])
        sh = [e[k] - dot3(p[k], w) for k in range(2)]
        c0 = [quantity(g, c) for c in range(9)]
        c1 = [quantity(g, 9 + c) for c in range(9)]
        for c in range(9):
            red[c, at, :] = c0[c] * sh[0] + c1[c] * sh[1]
        for pos, (i, j) in enumerate(PAIRS):
            if j == 0:
                a0 = k00 * c0[i] + k01 * c1[i]
                a1 = k01 * c0[i] + k11 * c1[i]
            ts[pl.ds(g * (8 * TS) + pos, 8, stride=TS), :] = a0 * c0[j] + a1 * c1[j]
        for pos in range(45, 48):
            ts[pl.ds(g * (8 * TS) + pos, 8, stride=TS), :] = jnp.zeros((8, 128), F32)

        cols, his, units = [], [], []
        for j in range(8):
            x = ts[pl.ds(m8(g * (8 * TS) + j * TS), 48), :]
            hi = x.astype(BF16)
            lo = (x - hi.astype(F32)).astype(BF16)
            slot = jnp.broadcast_to(slot_ref[pl.ds(g * 8 + j, 1), :], (16, 128))
            odd = (slot & 1).astype(BF16)
            lo4 = ((slot >> 1) & 15).astype(BF16)
            his.append((slot >> 5).astype(BF16))
            units.append(jnp.where(lo4 == iota16, one, zero))
            parts = []
            for y in (hi, lo):
                for par in (zero, one):
                    keep = odd == par
                    parts += [jnp.where(keep, y[16 * r : 16 * r + 16, :], zero) for r in range(3)]
                    parts += [zero]
            cols.append(jnp.concatenate(parts, axis=0))
        rhs = jnp.concatenate(cols, axis=1)
        rows = []
        for v in range(64):
            mine = jnp.full((16, 128), v, BF16)
            rows.append(
                jnp.concatenate([jnp.where(his[j] == mine, units[j], zero) for j in range(8)], axis=1)
            )
        lhs = jnp.concatenate(rows, axis=0)
        acc[...] += lax.dot_general(
            lhs, rhs, (((1,), (1,)), ((), ())), preferred_element_type=F32
        )
        return carry

    lax.fori_loop(0, 8, step, 0)


def invert(owned, ent, inv_ref):
    lane = lax.broadcasted_iota(I32, (128, 128), 1)
    wide = jnp.concatenate([owned] * 16, axis=0)
    spread = lane_pick(jnp.transpose(wide), (lane & 15) >> 1)
    ent[...] = jnp.where(lane[0:64] & 1 == 0, spread[0:64], spread[64:128])
    entry = {pair: ent[pl.ds(pos, 8, stride=0), :] for pos, pair in enumerate(PAIRS)}
    factor, recip = {}, {}
    for c in range(9):
        r = lax.rsqrt(entry[c, c] + 1.0 if c == 0 else entry[c, c])
        recip[c] = r
        for i in range(c + 1, 9):
            factor[i, c] = entry[i, c] * r
        for i in range(c + 1, 9):
            for j in range(c + 1, i + 1):
                base = entry[i, j] + 1.0 if (i == j and c == 0) else entry[i, j]
                entry[i, j] = base - factor[i, c] * factor[j, c]
    solved = {}
    for c in range(9):
        solved[c, c] = recip[c]
        for i in range(c + 1, 9):
            value = factor[i, c] * solved[c, c]
            for k in range(c + 1, i):
                value = value + factor[i, k] * solved[k, c]
            solved[i, c] = -value * recip[i]
    row8 = lax.broadcasted_iota(I32, (8, 128), 0)
    lane8 = lax.broadcasted_iota(I32, (8, 128), 1)
    tile = jnp.zeros((8, 128), F32)
    for pos, (i, j) in enumerate(PAIRS):
        value = solved[i, i] * solved[i, j]
        for k in range(i + 1, 9):
            value = value + solved[k, i] * solved[k, j]
        inv_ref[9 * i + j : 9 * i + j + 1, :] = value[0:1, 0:16]
        if i != j:
            inv_ref[9 * j + i : 9 * j + i + 1, :] = value[0:1, 0:16]
        tile = jnp.where((row8 == pos // 8) & (lane8 // 16 == pos % 8), value, tile)
    return tile


def arrange(tiles, table):
    lane = lax.broadcasted_iota(I32, (8, 128), 1)

    def step(h, carry):
        x = [tiles[h * 8 + e] for e in range(8)]
        for k in (1, 2, 4):
            upper = (lane // 16) & k != 0
            for e in range(8):
                if e & k == 0:
                    low, high = x[e], x[e + k]
                    x[e] = jnp.where(upper, pltpu.roll(high, 16 * k, 1), low)
                    x[e + k] = jnp.where(upper, high, pltpu.roll(low, 128 - 16 * k, 1))
        for b in range(8):
            table[h, 8 * b : 8 * b + 8, :] = x[b]
        return carry

    lax.fori_loop(0, 16, step, 0)


def apply_inverses(table, slot_ref, red, outs, out_ref):
    def step(g, carry):
        at = pl.ds(m8(g * 8), 8)
        slot = slot_ref[at, :]
        lo = slot & 127
        bits = [((slot >> (7 + b)) & 1) == 1 for b in range(4)]
        part = [red[c, at, :] for c in range(9)]
        total = [None] * 9
        for pos, (i, j) in enumerate(PAIRS):
            row = 8 * (pos % 8) + pos // 8
            vals = [lane_pick(table[h, pl.ds(row, 8, stride=0), :], lo) for h in range(16)]
            for b in range(4):
                vals = [jnp.where(bits[b], vals[2 * n + 1], vals[2 * n]) for n in range(len(vals) // 2)]
            for r, c in sorted({(i, j), (j, i)}):
                x = vals[0] * part[c]
                total[r] = x if total[r] is None else total[r] + x
        for r in range(9):
            outs[pl.ds(g * (8 * OS) + r, 8, stride=OS), :] = total[r]
        return carry

    lax.fori_loop(0, 8, step, 0)
    for j in range(64):
        at = pl.ds(j * 128, 128)
        out_ref[0:8, at] = outs[j * OS : j * OS + 8, :]
        out_ref[8:9, at] = outs[j * OS + 8 : j * OS + 9, :]


def kernel(cam_ref, pt_ref, res_ref, pid_ref, cid_ref, map_ref, inv_ref, out_ref,
           slot_ref, xs, ts, tot, heads, tails, fix, acc, red, ent, outs, table,
           part, swap, half, recv, owned, tiles, swap_sems, send_sems, recv_sems):
    pts, core = lax.axis_index("pts"), lax.axis_index("grp")
    partner = (pts, 1 - core)

    def chip(off):
        z, x, y = pts // 16, pts // 4 % 4, pts % 4
        return ((z + off // 16) % 4) * 16 + ((x + off // 4 % 4) % 4) * 4 + (y + off % 4) % 4

    barrier = pltpu.get_barrier_semaphore()
    pl.semaphore_signal(barrier, inc=1, device_id=partner, device_id_type=MESH)
    for off in range(1, CHIPS):
        pl.semaphore_signal(barrier, inc=1, device_id=(chip(off), core), device_id_type=MESH)

    find_slots(cid_ref, map_ref, slot_ref)
    spread_inputs(cam_ref, pt_ref, res_ref, xs)
    point_sums(pid_ref, xs, tot, heads, tails, fix)
    camera_sums(pid_ref, slot_ref, xs, tot, fix, red, ts, acc)

    def fold(n, carry):
        at = pl.ds(m8(n * 16), 16)
        part[n] = (acc[at, 0:128] + acc[at, 128:256]).reshape(2, 8, 128)
        return carry

    lax.fori_loop(0, CHIPS, fold, 0)
    pl.semaphore_wait(barrier, CHIPS)

    copy = pltpu.make_async_remote_copy(
        src_ref=part.at[:, 1 - core], dst_ref=swap, send_sem=swap_sems.at[0],
        recv_sem=swap_sems.at[1], device_id=partner, device_id_type=MESH)
    copy.start()
    copy.wait()

    def join(n, carry):
        half[n] = part[n, core] + swap[n]
        return carry

    lax.fori_loop(0, CHIPS, join, 0)
    for off in OFFSETS:
        to = chip(off)
        pltpu.make_async_remote_copy(
            src_ref=half.at[to], dst_ref=recv.at[off - 1], send_sem=send_sems.at[0],
            recv_sem=recv_sems.at[0], device_id=(to, core), device_id_type=MESH).start()
    arrived = pltpu.make_async_copy(recv, recv, recv_sems.at[0])
    arrived.wait()
    pltpu.make_async_copy(recv, recv, send_sems.at[0]).wait()

    sums = [recv[n] for n in range(CHIPS - 1)] + [half[pts]]
    while len(sums) > 1:
        sums = [sums[i] + sums[i + 1] for i in range(0, len(sums) - 1, 2)] + sums[len(sums) & ~1 :]
    owned[...] = invert(sums[0], ent, inv_ref)
    tiles[pts, core] = owned[...]

    for off in OFFSETS:
        pltpu.make_async_remote_copy(
            src_ref=owned, dst_ref=tiles.at[pts, core], send_sem=send_sems.at[1],
            recv_sem=recv_sems.at[1], device_id=(chip(off), core), device_id_type=MESH).start()
    pltpu.make_async_copy(recv, recv, recv_sems.at[1]).wait()
    pltpu.make_async_copy(recv, recv, send_sems.at[1]).wait()
    copy = pltpu.make_async_remote_copy(
        src_ref=tiles.at[:, core], dst_ref=tiles.at[:, core], send_sem=swap_sems.at[2],
        recv_sem=swap_sems.at[3], device_id=partner, device_id_type=MESH)
    copy.start()
    copy.wait()
    arrange(tiles.reshape(2 * CHIPS, 8, 128), table)
    apply_inverses(table, slot_ref, red, outs, out_ref)


def shards(cam_jac, pt_jac, resid, obs_point, obs_camera, camera_slot):
    vm = pltpu.VMEM
    dma = pltpu.SemaphoreType.DMA
    return pl.pallas_call(
        kernel,
        out_shape=(jax.ShapeDtypeStruct((81, 16), F32), jax.ShapeDtypeStruct((9, 8192), F32)),
        in_specs=[pl.BlockSpec(memory_space=vm)] * 6,
        out_specs=(pl.BlockSpec(memory_space=vm), pl.BlockSpec(memory_space=vm)),
        scratch_shapes=[
            vm((64, 128), I32),
            vm((64 * XS, 128), F32),
            vm((64 * TS, 128), F32),
            vm((9 * 64, 128), F32),
            vm((64, 128), F32),
            vm((64, 128), F32),
            vm((128, 128), F32),
            vm((1024, 256), F32),
            vm((9, 64, 128), F32),
            vm((64, 128), F32),
            vm((64 * OS, 128), F32),
            vm((16, 64, 128), F32),
            vm((CHIPS, 2, 8, 128), F32),
            vm((CHIPS, 8, 128), F32),
            vm((CHIPS, 8, 128), F32),
            vm((CHIPS - 1, 8, 128), F32),
            vm((8, 128), F32),
            vm((CHIPS, 2, 8, 128), F32),
            dma((4,)),
            dma((2,)),
            dma((2,)),
        ],
        compiler_params=pltpu.CompilerParams(
            vmem_limit_bytes=58 * 2**20, collective_id=0, has_side_effects=True
        ),
        name="schur",
    )(
        cam_jac,
        pt_jac,
        resid,
        obs_point.reshape(64, 128),
        obs_camera.reshape(64, 128),
        camera_slot.reshape(16, 128),
    )


def solution(mesh):
    both = ("pts", "grp")
    in_specs = (P(None, both), P(None, both), P(None, both), P(both), P(both), P())
    out_specs = (P(None, both), P(None, both))
    return jax.shard_map(shards, mesh=mesh, in_specs=in_specs, out_specs=out_specs, check_vma=False)
```

```python
import jax
import jax.numpy as jnp
from jax import lax
from jax.experimental import pallas as pl
from jax.experimental.pallas import tpu as pltpu
from jax.sharding import PartitionSpec as P

F32, BF16, I32 = jnp.float32, jnp.bfloat16, jnp.int32
MESH = pl.DeviceIdType.MESH
XS = 40
TS = 56
OS = 24
PS = 40
PAIRS = [(i, j) for i in range(9) for j in range(i + 1)]
CHIPS = 64


def hops(off):
    return sum(min(d, 4 - d) for d in (off // 16, off // 4 % 4, off % 4))


OFFSETS = sorted(range(1, CHIPS), key=lambda off: (-hops(off), off))


def m8(x):
    return pl.multiple_of(x, 8)


def lane_pick(row, idx):
    return jnp.take_along_axis(row, idx, axis=1, mode="promise_in_bounds")


def find_slots(cid_ref, map_ref, slot_ref):
    for g in range(8):
        cid = cid_ref[g * 8 : g * 8 + 8, :]
        lo = cid & 127
        vals = [lane_pick(map_ref[pl.ds(h, 8, stride=0), :], lo) for h in range(16)]
        for b in range(4):
            bit = ((cid >> (7 + b)) & 1) == 1
            vals = [jnp.where(bit, vals[2 * i + 1], vals[2 * i]) for i in range(len(vals) // 2)]
        slot_ref[g * 8 : g * 8 + 8, :] = vals[0]


def spread_points(pt_ref, res_ref, xs):
    for j in range(64):
        at = pl.ds(j * 128, 128)
        xs[j * XS + 24 : j * XS + 30, :] = pt_ref[0:6, at]
        xs[j * XS + 32 : j * XS + 34, :] = res_ref[0:2, at]


def spread_cameras(cam_ref, xs):
    for j in range(64):
        at = pl.ds(j * 128, 128)
        xs[j * XS : j * XS + 8, :] = cam_ref[0:8, at]
        xs[j * XS + 8 : j * XS + 16, :] = cam_ref[8:16, at]
        xs[j * XS + 16 : j * XS + 18, :] = cam_ref[16:18, at]


def point_sums(pid_ref, xs, tot, heads, tails, fix):
    lane = lax.broadcasted_iota(I32, (8, 128), 1)

    def quantity(g, q):
        return xs[pl.ds(g * (8 * XS) + q, 8, stride=XS), :]

    def one(g):
        p = [[quantity(g, 24 + 3 * k + c) for c in range(3)] for k in range(2)]
        e = [quantity(g, 32 + k) for k in range(2)]
        pid = pid_ref[pl.ds(m8(g * 8), 8), :]
        v = [p[0][a] * p[0][c] + p[1][a] * p[1][c] for a in range(3) for c in range(a, 3)]
        v += [p[0][a] * e[0] + p[1][a] * e[1] for a in range(3)]
        return pid, v, lane

    def scan(state, k):
        pid, v, end = state
        same = (pltpu.roll(pid, k, 1) == pid) & (lane >= k)
        v = [x + jnp.where(same, pltpu.roll(x, k, 1), 0.0) for x in v]
        after = (pltpu.roll(pid, 128 - k, 1) == pid) & (lane < 128 - k)
        return pid, v, jnp.where(after, pltpu.roll(end, 128 - k, 1), end)

    def finish(g, state):
        pid, v, end = state
        head = jnp.zeros((8, 128), F32)
        tail = jnp.zeros((8, 128), F32)
        for q in range(9):
            full = lane_pick(v[q], end)
            tot[pl.ds(m8(q * 64 + g * 8), 8), :] = full
            head = jnp.where(lane == q, jnp.broadcast_to(full[:, 0:1], (8, 128)), head)
            tail = jnp.where(lane == q, jnp.broadcast_to(full[:, 127:128], (8, 128)), tail)
        heads[pl.ds(m8(g * 8), 8), :] = head
        tails[pl.ds(m8(g * 8), 8), :] = tail

    def step(n, carry):
        states = [one(n * 4 + u) for u in range(4)]
        for b in range(7):
            states = [scan(state, 1 << b) for state in states]
        for u in range(4):
            finish(n * 4 + u, states[u])
        return carry

    lax.fori_loop(0, 2, step, 0)

    pid = pid_ref[...]
    first = jnp.broadcast_to(pid[:, 0:1], (64, 128))
    last = jnp.broadcast_to(pid[:, 127:128], (64, 128))
    ends = jnp.where(lax.broadcasted_iota(I32, (64, 128), 1) < 64, first, last).astype(F32)
    across = jnp.transpose(ends)
    r0 = lax.broadcasted_iota(I32, (64, 64), 0)
    r1 = lax.broadcasted_iota(I32, (64, 64), 1)
    from_before = (r1 < r0) & (across[64:128, :] == first[:, 0:64].astype(F32))
    from_after = (r1 > r0) & (across[0:64, :] == last[:, 0:64].astype(F32))

    def total(which, values):
        return lax.dot_general(
            jnp.where(which, 1.0, 0.0),
            values[...],
            (((1,), (0,)), ((), ())),
            precision=lax.Precision.HIGHEST,
            preferred_element_type=F32,
        )

    fix[0:64, :] = total(from_before, tails)
    fix[64:128, :] = total(from_after, heads)


def camera_sums(pid_ref, slot_ref, xs, tot, fix, red, ts, rhs, acc):
    def quantity(g, q):
        return xs[pl.ds(g * (8 * XS) + q, 8, stride=XS), :]

    def dot3(a, b):
        return a[0] * b[0] + a[1] * b[1] + a[2] * b[2]

    zero = jnp.zeros((16, 128), BF16)
    one = jnp.ones((16, 128), BF16)

    def terms(g):
        at = pl.ds(g * 8, 8)
        pid = pid_ref[at, :]
        pre = fix[at, :]
        post = fix[pl.ds(64 + g * 8, 8), :]
        is_first = pid == jnp.broadcast_to(pid[:, 0:1], (8, 128))
        is_last = pid == jnp.broadcast_to(pid[:, 127:128], (8, 128))
        s = []
        for q in range(9):
            x = tot[pl.ds(q * 64 + g * 8, 8), :]
            x = x + jnp.where(is_first, jnp.broadcast_to(pre[:, q : q + 1], (8, 128)), 0.0)
            x = x + jnp.where(is_last, jnp.broadcast_to(post[:, q : q + 1], (8, 128)), 0.0)
            s.append(x)
        v00, v01, v02, v11, v12, v22 = s[0] + 1.0, s[1], s[2], s[3] + 1.0, s[4], s[5] + 1.0
        c00 = v11 * v22 - v12 * v12
        c01 = v02 * v12 - v01 * v22
        c02 = v01 * v12 - v02 * v11
        c11 = v00 * v22 - v02 * v02
        c12 = v01 * v02 - v00 * v12
        c22 = v00 * v11 - v01 * v01
        inv = 1.0 / (v00 * c00 + v01 * c01 + v02 * c02)
        i00, i01, i02, i11, i12, i22 = [c * inv for c in (c00, c01, c02, c11, c12, c22)]
        vinv = ((i00, i01, i02), (i01, i11, i12), (i02, i12, i22))
        w = [dot3(vinv[a], s[6:9]) for a in range(3)]
        p = [[quantity(g, 24 + 3 * k + c) for c in range(3)] for k in range(2)]
        e = [quantity(g, 32 + k) for k in range(2)]
        use = [[dot3(vinv[a], p[k]) for a in range(3)] for k in range(2)]
        k00 = 1.0 - dot3(p[0], use[0])
        k01 = -dot3(p[0], use[1])
        k11 = 1.0 - dot3(p[1], use[1])
        sh = [e[k] - dot3(p[k], w) for k in range(2)]
        c0 = [quantity(g, c) for c in range(9)]
        c1 = [quantity(g, 9 + c) for c in range(9)]
        for c in range(9):
            red[c, at, :] = c0[c] * sh[0] + c1[c] * sh[1]
        base = (g % 2) * (8 * TS)
        for pos, (i, j) in enumerate(PAIRS):
            if j == 0:
                a0 = k00 * c0[i] + k01 * c1[i]
                a1 = k01 * c0[i] + k11 * c1[i]
            ts[pl.ds(base + pos, 8, stride=TS), :] = a0 * c0[j] + a1 * c1[j]
        for pos in range(45, 48):
            ts[pl.ds(base + pos, 8, stride=TS), :] = jnp.zeros((8, 128), F32)

        for j in range(8):
            x = ts[base + j * TS : base + j * TS + 48, :]
            hi = x.astype(BF16)
            lo = (x - hi.astype(F32)).astype(BF16)
            slot = jnp.broadcast_to(slot_ref[g * 8 + j : g * 8 + j + 1, :], (16, 128))
            odd = (slot & 1).astype(BF16)
            parts = []
            for y in (hi, lo):
                for par in (zero, one):
                    keep = odd == par
                    parts += [jnp.where(keep, y[16 * r : 16 * r + 16, :], zero) for r in range(3)]
                    parts += [zero]
            rhs[g % 2, :, j * 128 : j * 128 + 128] = jnp.concatenate(parts, axis=0)

    def multiply(g):
        lhs = one_hot(slot_ref, g, 1, 64)
        part = lax.dot_general(
            lhs, rhs[g % 2], (((1,), (1,)), ((), ())), preferred_element_type=F32
        )
        acc[...] = part if g == 0 else acc[...] + part

    terms(0)
    for g in range(8):
        multiply(g)
        if g < 7:
            terms(g + 1)


def one_hot(slot_ref, g, shift, groups):
    iota = lax.broadcasted_iota(I32, (16, 128), 0).astype(BF16)
    zero = jnp.zeros((16, 128), BF16)
    one = jnp.ones((16, 128), BF16)
    unit, group = [], []
    for j in range(8):
        slot = jnp.broadcast_to(slot_ref[pl.ds(g * 8 + j, 1), :], (16, 128))
        unit.append(jnp.where(((slot >> shift) & 15).astype(BF16) == iota, one, zero))
        group.append(((slot >> (shift + 4)) & (groups - 1)).astype(BF16))
    rows = []
    for v in range(groups):
        mine = jnp.full((16, 128), v, BF16)
        rows.append(jnp.concatenate([jnp.where(group[j] == mine, unit[j], zero) for j in range(8)], axis=1))
    return jnp.concatenate(rows, axis=0)


def invert(owned, ent, inv_ref):
    lane = lax.broadcasted_iota(I32, (128, 128), 1)
    wide = jnp.concatenate([owned] * 16, axis=0)
    spread = lane_pick(jnp.transpose(wide), (lane & 15) >> 1)
    ent[...] = jnp.where(lane[0:64] & 1 == 0, spread[0:64], spread[64:128])
    entry = {pair: ent[pl.ds(pos, 8, stride=0), :] for pos, pair in enumerate(PAIRS)}
    factor, recip = {}, {}
    for c in range(9):
        r = lax.rsqrt(entry[c, c] + 1.0 if c == 0 else entry[c, c])
        recip[c] = r
        for i in range(c + 1, 9):
            factor[i, c] = entry[i, c] * r
        for i in range(c + 1, 9):
            for j in range(c + 1, i + 1):
                base = entry[i, j] + 1.0 if (i == j and c == 0) else entry[i, j]
                entry[i, j] = base - factor[i, c] * factor[j, c]
    solved = {}
    for c in range(9):
        solved[c, c] = recip[c]
        for i in range(c + 1, 9):
            value = factor[i, c] * solved[c, c]
            for k in range(c + 1, i):
                value = value + factor[i, k] * solved[k, c]
            solved[i, c] = -value * recip[i]
    row8 = lax.broadcasted_iota(I32, (8, 128), 0)
    lane8 = lax.broadcasted_iota(I32, (8, 128), 1)
    tile = jnp.zeros((8, 128), F32)
    for pos, (i, j) in enumerate(PAIRS):
        value = solved[i, i] * solved[i, j]
        for k in range(i + 1, 9):
            value = value + solved[k, i] * solved[k, j]
        inv_ref[9 * i + j : 9 * i + j + 1, :] = value[0:1, :]
        if i != j:
            inv_ref[9 * j + i : 9 * j + i + 1, :] = value[0:1, :]
        tile = jnp.where((row8 == pos % 8) & (lane8 // 16 == pos // 8), value, tile)
    return tile


def arrange(tiles, table, left):
    lane = lax.broadcasted_iota(I32, (8, 128), 1)
    for h in range(16):
        x = [tiles[h * 8 + e] for e in range(8)]
        for k in (1, 2, 4):
            upper = (lane // 16) & k != 0
            for e in range(8):
                if e & k == 0:
                    low, high = x[e], x[e + k]
                    x[e] = jnp.where(upper, pltpu.roll(high, 16 * k, 1), low)
                    x[e + k] = jnp.where(upper, high, pltpu.roll(low, 128 - 16 * k, 1))
        for b in (4, 5):
            table[h, 8 * (b - 4) : 8 * (b - 4) + 8, :] = x[b]
        values = jnp.concatenate(x[0:4], axis=0)
        hi = values.astype(BF16)
        lo = (values - hi.astype(F32)).astype(BF16)
        at = pl.ds(128 * (h % 4), 128)
        left[64 * (h // 4) : 64 * (h // 4) + 32, at] = hi
        left[64 * (h // 4) + 32 : 64 * (h // 4) + 64, at] = lo


def apply_inverses(table, left, slot_ref, red_ref, picked, outs, out_ref):
    for g in range(8):
        at = pl.ds(g * 8, 8)
        slot = slot_ref[at, :]
        lo = slot & 127
        bits = [((slot >> (7 + b)) & 1) == 1 for b in range(4)]
        part = [red_ref[c, at, :] for c in range(9)]
        chosen = lax.dot_general(
            left[...], one_hot(slot_ref, g, 0, 32), (((1,), (0,)), ((), ())), preferred_element_type=F32
        )
        base = (g % 2) * (8 * PS)
        for j in range(8):
            quarter = jnp.broadcast_to(slot_ref[g * 8 + j : g * 8 + j + 1, :], (8, 128)) >> 9
            low, high = (quarter & 1) == 1, quarter > 1
            for r in range(0, 32, 8):
                y = [chosen[64 * q + r : 64 * q + r + 8, 128 * j : 128 * j + 128]
                     + chosen[64 * q + 32 + r : 64 * q + 40 + r, 128 * j : 128 * j + 128] for q in range(4)]
                picked[base + PS * j + r : base + PS * j + r + 8, :] = jnp.where(
                    high, jnp.where(low, y[3], y[2]), jnp.where(low, y[1], y[0]))
        total = [None] * 9
        for pos, (i, j) in enumerate(PAIRS):
            if pos < 32:
                value = picked[pl.ds(base + pos, 8, stride=PS), :]
            else:
                vals = [lane_pick(table[h, pl.ds(pos - 32, 8, stride=0), :], lo) for h in range(16)]
                for b in range(4):
                    vals = [jnp.where(bits[b], vals[2 * n + 1], vals[2 * n]) for n in range(len(vals) // 2)]
                value = vals[0]
            for r, c in sorted({(i, j), (j, i)}):
                x = value * part[c]
                total[r] = x if total[r] is None else total[r] + x
        base = (g % 2) * (8 * OS)
        for r in range(9):
            outs[pl.ds(base + r, 8, stride=OS), :] = total[r]
        for j in range(8):
            at = pl.ds((g * 8 + j) * 128, 128)
            out_ref[0:8, at] = outs[base + j * OS : base + j * OS + 8, :]
            out_ref[8:9, at] = outs[base + j * OS + 8 : base + j * OS + 9, :]


def last(tiles, slot_ref, red_ref, rows_ref, inv_ref, out_ref, table, left, picked, outs):
    arrange(tiles, table, left)
    inv_ref[...] = jnp.transpose(rows_ref[...])[0:16, 0:81]
    apply_inverses(table, left, slot_ref, red_ref, picked, outs, out_ref)


def kernel(cam_hbm, pt_hbm, res_hbm, pid_hbm, cid_hbm, map_hbm, tiles, slot_ref, red, rows_ref,
           cam_ref, pt_ref, res_ref, pid_ref, cid_ref, map_ref,
           xs, ts, tot, heads, tails, fix, rhs, acc, ent,
           part, swap, half, recv, owned, load_sems, swap_sems, send_sems, recv_sems):
    pts, core = lax.axis_index("pts"), lax.axis_index("grp")
    partner = (pts, 1 - core)

    def chip(off):
        z, x, y = pts // 16, pts // 4 % 4, pts % 4
        return ((z + off // 16) % 4) * 16 + ((x + off // 4 % 4) % 4) * 4 + (y + off % 4) % 4

    pairs = [(cid_hbm, cid_ref), (map_hbm, map_ref), (pid_hbm, pid_ref), (pt_hbm, pt_ref),
             (res_hbm, res_ref), (cam_hbm, cam_ref)]
    loads = [pltpu.make_async_copy(src, dst, load_sems.at[n]) for n, (src, dst) in enumerate(pairs)]
    for load in loads:
        load.start()
    barrier = pltpu.get_barrier_semaphore()
    pl.semaphore_signal(barrier, inc=1, device_id=partner, device_id_type=MESH)
    for off in range(1, CHIPS):
        pl.semaphore_signal(barrier, inc=1, device_id=(chip(off), core), device_id_type=MESH)

    with jax.named_scope("load"):
        for load in loads[0:2]:
            load.wait()
    with jax.named_scope("slots"):
        find_slots(cid_ref, map_ref, slot_ref)
        for load in loads[2:5]:
            load.wait()
        spread_points(pt_ref, res_ref, xs)
    with jax.named_scope("points"):
        point_sums(pid_ref, xs, tot, heads, tails, fix)
    with jax.named_scope("cameras"):
        loads[5].wait()
        spread_cameras(cam_ref, xs)
        camera_sums(pid_ref, slot_ref, xs, tot, fix, red, ts, rhs, acc)

    with jax.named_scope("fold"):
        for n in range(CHIPS):
            at = pl.ds(n * 16, 16)
            part[n] = (acc[at, 0:128] + acc[at, 128:256]).reshape(2, 8, 128)
    with jax.named_scope("barrier"):
        pl.semaphore_wait(barrier, CHIPS)

    with jax.named_scope("swap"):
        copy = pltpu.make_async_remote_copy(
            src_ref=part.at[:, 1 - core], dst_ref=swap, send_sem=swap_sems.at[0],
            recv_sem=swap_sems.at[1], device_id=partner, device_id_type=MESH)
        copy.start()
        copy.wait()

    with jax.named_scope("scatter"):
        for n in range(CHIPS):
            half[n] = part[n, core] + swap[n]
        for off in OFFSETS:
            to = chip(off)
            pltpu.make_async_remote_copy(
                src_ref=half.at[to], dst_ref=recv.at[off - 1], send_sem=send_sems.at[0],
                recv_sem=recv_sems.at[0], device_id=(to, core), device_id_type=MESH).start()
        pltpu.make_async_copy(recv, recv, recv_sems.at[0]).wait()

    with jax.named_scope("invert"):
        sums = [recv[n] for n in range(CHIPS - 1)] + [half[pts]]
        while len(sums) > 1:
            sums = [sums[i] + sums[i + 1] for i in range(0, len(sums) - 1, 2)] + sums[len(sums) & ~1 :]
        owned[...] = invert(sums[0], ent, rows_ref)
        tiles[pts, core] = owned[...]

    with jax.named_scope("gather"):
        for off in OFFSETS:
            pltpu.make_async_remote_copy(
                src_ref=owned, dst_ref=tiles.at[pts, core], send_sem=send_sems.at[1],
                recv_sem=recv_sems.at[1], device_id=(chip(off), core), device_id_type=MESH).start()
        pltpu.make_async_copy(recv, recv, recv_sems.at[1]).wait()
    with jax.named_scope("across"):
        copy = pltpu.make_async_remote_copy(
            src_ref=tiles.at[:, core], dst_ref=tiles.at[:, core], send_sem=swap_sems.at[2],
            recv_sem=swap_sems.at[3], device_id=partner, device_id_type=MESH)
        copy.start()
        pltpu.make_async_copy(recv, recv, send_sems.at[0]).wait()
        pltpu.make_async_copy(recv, recv, send_sems.at[1]).wait()
        copy.wait()


def shards(cam_jac, pt_jac, resid, obs_point, obs_camera, camera_slot):
    vm = pltpu.VMEM
    dma = pltpu.SemaphoreType.DMA
    shape = jax.ShapeDtypeStruct
    tiles, slots, red, rows = pl.pallas_call(
        kernel,
        out_shape=(
            shape((CHIPS, 2, 8, 128), F32),
            shape((64, 128), I32),
            shape((9, 64, 128), F32),
            shape((128, 128), F32),
        ),
        in_specs=[pl.BlockSpec(memory_space=pltpu.HBM)] * 6,
        out_specs=[pl.BlockSpec(memory_space=vm)] * 4,
        scratch_shapes=[
            vm((18, 8192), F32),
            vm((6, 8192), F32),
            vm((2, 8192), F32),
            vm((64, 128), I32),
            vm((64, 128), I32),
            vm((16, 128), I32),
            vm((64 * XS, 128), F32),
            vm((16 * TS, 128), F32),
            vm((9 * 64, 128), F32),
            vm((64, 128), F32),
            vm((64, 128), F32),
            vm((128, 128), F32),
            vm((2, 256, 1024), BF16),
            vm((1024, 256), F32),
            vm((64, 128), F32),
            vm((CHIPS, 2, 8, 128), F32),
            vm((CHIPS, 8, 128), F32),
            vm((CHIPS, 8, 128), F32),
            vm((CHIPS - 1, 8, 128), F32),
            vm((8, 128), F32),
            dma((6,)),
            dma((4,)),
            dma((2,)),
            dma((2,)),
        ],
        compiler_params=pltpu.CompilerParams(
            vmem_limit_bytes=28 * 2**20, collective_id=0, has_side_effects=True
        ),
        name="schur",
    )(
        *[
            pltpu.with_memory_space_constraint(x, pltpu.HBM)
            for x in (
                cam_jac,
                pt_jac,
                resid,
                obs_point.reshape(64, 128),
                obs_camera.reshape(64, 128),
                camera_slot.reshape(16, 128),
            )
        ]
    )
    inverse, precond = pl.pallas_call(
        last,
        out_shape=(shape((16, 81), F32), shape((9, 8192), F32)),
        in_specs=[pl.BlockSpec(memory_space=vm)] * 4,
        out_specs=[pl.BlockSpec(memory_space=vm)] * 2,
        scratch_shapes=[
            vm((16, 16, 128), F32),
            vm((256, 512), BF16),
            vm((16 * PS, 128), F32),
            vm((16 * OS, 128), F32),
        ],
        compiler_params=pltpu.CompilerParams(vmem_limit_bytes=28 * 2**20),
        name="last",
    )(tiles.reshape(2 * CHIPS, 8, 128), slots, red, rows)
    return inverse.T, precond


def solution(mesh):
    both = ("pts", "grp")
    in_specs = (P(None, both), P(None, both), P(None, both), P(both), P(both), P())
    out_specs = (P(None, both), P(None, both))
    return jax.shard_map(shards, mesh=mesh, in_specs=in_specs, out_specs=out_specs, check_vma=False)
```

```python
import jax
import jax.numpy as jnp
import numpy as np
from jax import lax
from jax.experimental import pallas as pl
from jax.experimental.pallas import tpu as pltpu
from jax.sharding import PartitionSpec as P

F32, BF16, I32 = jnp.float32, jnp.bfloat16, jnp.int32
MESH = pl.DeviceIdType.MESH
XS = 40
TS = 56
OS = 24
PS = 56
PAIRS = [(i, j) for i in range(9) for j in range(i + 1)]
CHIPS = 64


def hops(off):
    return sum(min(d, 4 - d) for d in (off // 16, off // 4 % 4, off % 4))


OFFSETS = sorted(range(CHIPS), key=lambda off: (-hops(off), off))
RANK = {off: r for r, off in enumerate(OFFSETS)}
PARTS = 4
EACH = CHIPS // PARTS


def back(off):
    return ((-(off >> 4) & 3) << 4) | ((-(off >> 2) & 3) << 2) | (-off & 3)


def m8(x):
    return pl.multiple_of(x, 8)


def lane_pick(row, idx):
    return jnp.take_along_axis(row, idx, axis=1, mode="promise_in_bounds")


def find_slots(pts, core, cid_ref, map_ref, rank_ref, pos_ref, pick_ref):
    z, x, y = pts >> 4, (pts >> 2) & 3, pts & 3
    rank = rank_ref[...]
    for g in range(8):
        cid = cid_ref[g * 8 : g * 8 + 8, :]
        lo = cid & 127
        vals = [lane_pick(map_ref[pl.ds(h, 8, stride=0), :], lo) for h in range(16)]
        for b in range(4):
            bit = ((cid >> (7 + b)) & 1) == 1
            vals = [jnp.where(bit, vals[2 * i + 1], vals[2 * i]) for i in range(len(vals) // 2)]
        slot = vals[0]
        off = ((((slot >> 9) - z) & 3) << 4) | ((((slot >> 7) - x) & 3) << 2) | (((slot >> 5) - y) & 3)
        near = lane_pick(rank, off)
        pos_ref[g * 8 : g * 8 + 8, :] = (near << 5) | (slot & 31)
        pick_ref[g * 8 : g * 8 + 8, :] = ((((slot >> 4) & 1) ^ core) << 10) | (near << 4) | (slot & 15)


def spread_points(pt_ref, res_ref, xs):
    for j in range(64):
        at = pl.ds(j * 128, 128)
        xs[j * XS + 24 : j * XS + 30, :] = pt_ref[0:6, at]
        xs[j * XS + 32 : j * XS + 34, :] = res_ref[0:2, at]


def spread_cameras(cam_ref, xs):
    for j in range(64):
        at = pl.ds(j * 128, 128)
        xs[j * XS : j * XS + 8, :] = cam_ref[0:8, at]
        xs[j * XS + 8 : j * XS + 16, :] = cam_ref[8:16, at]
        xs[j * XS + 16 : j * XS + 18, :] = cam_ref[16:18, at]


def point_sums(pid_ref, xs, tot, heads, tails, fix, between):
    lane = lax.broadcasted_iota(I32, (8, 128), 1)

    def quantity(g, q):
        return xs[pl.ds(g * (8 * XS) + q, 8, stride=XS), :]

    def one(g):
        p = [[quantity(g, 24 + 3 * k + c) for c in range(3)] for k in range(2)]
        e = [quantity(g, 32 + k) for k in range(2)]
        pid = pid_ref[pl.ds(m8(g * 8), 8), :]
        v = [p[0][a] * p[0][c] + p[1][a] * p[1][c] for a in range(3) for c in range(a, 3)]
        v += [p[0][a] * e[0] + p[1][a] * e[1] for a in range(3)]
        return pid, v, lane

    def scan(state, k):
        pid, v, end = state
        same = (pltpu.roll(pid, k, 1) == pid) & (lane >= k)
        v = [x + jnp.where(same, pltpu.roll(x, k, 1), 0.0) for x in v]
        after = (pltpu.roll(pid, 128 - k, 1) == pid) & (lane < 128 - k)
        return pid, v, jnp.where(after, pltpu.roll(end, 128 - k, 1), end)

    def finish(g, state):
        pid, v, end = state
        head = jnp.zeros((8, 128), F32)
        tail = jnp.zeros((8, 128), F32)
        for q in range(9):
            full = lane_pick(v[q], end)
            tot[pl.ds(m8(q * 64 + g * 8), 8), :] = full
            ends = pltpu.roll(full, q + 1, 1)
            head = jnp.where(lane == q + 1, ends, head)
            tail = jnp.where(lane == q, ends, tail)
        heads[pl.ds(m8(g * 8), 8), :] = head
        tails[pl.ds(m8(g * 8), 8), :] = tail

    def step(n, carry):
        states = [one(n * 4 + u) for u in range(4)]
        for b in range(7):
            states = [scan(state, 1 << b) for state in states]
        for u in range(4):
            finish(n * 4 + u, states[u])
        return carry

    lax.fori_loop(0, 2, step, 0)
    between()

    pid = pid_ref[...]
    first = jnp.broadcast_to(pid[:, 0:1], (64, 128))
    last = jnp.broadcast_to(pid[:, 127:128], (64, 128))
    ends = jnp.where(lax.broadcasted_iota(I32, (64, 128), 1) < 64, first, last).astype(F32)
    across = jnp.transpose(ends)
    r0 = lax.broadcasted_iota(I32, (64, 64), 0)
    r1 = lax.broadcasted_iota(I32, (64, 64), 1)
    from_before = (r1 < r0) & (across[64:128, :] == first[:, 0:64].astype(F32))
    from_after = (r1 > r0) & (across[0:64, :] == last[:, 0:64].astype(F32))

    def total(which, values):
        return lax.dot_general(
            jnp.where(which, 1.0, 0.0),
            values[...],
            (((1,), (0,)), ((), ())),
            precision=lax.Precision.HIGHEST,
            preferred_element_type=F32,
        )

    fix[0:64, :] = total(from_before, tails)
    fix[64:128, :] = total(from_after, heads)


def camera_sums(pid_ref, slot_ref, xs, tot, fix, red, ts, rhs, acc, done, send):
    def quantity(g, q):
        return xs[pl.ds(g * (8 * XS) + q, 8, stride=XS), :]

    def dot3(a, b):
        return a[0] * b[0] + a[1] * b[1] + a[2] * b[2]

    def terms(g):
        at = pl.ds(g * 8, 8)
        pid = pid_ref[at, :]
        pre = fix[at, :]
        post = fix[pl.ds(64 + g * 8, 8), :]
        is_first = pid == jnp.broadcast_to(pid[:, 0:1], (8, 128))
        is_last = pid == jnp.broadcast_to(pid[:, 127:128], (8, 128))
        s = []
        for q in range(9):
            x = tot[pl.ds(q * 64 + g * 8, 8), :]
            x = x + jnp.where(is_first, jnp.broadcast_to(pre[:, q : q + 1], (8, 128)), 0.0)
            x = x + jnp.where(is_last, jnp.broadcast_to(post[:, q + 1 : q + 2], (8, 128)), 0.0)
            s.append(x)
        v00, v01, v02, v11, v12, v22 = s[0] + 1.0, s[1], s[2], s[3] + 1.0, s[4], s[5] + 1.0
        c00 = v11 * v22 - v12 * v12
        c01 = v02 * v12 - v01 * v22
        c02 = v01 * v12 - v02 * v11
        c11 = v00 * v22 - v02 * v02
        c12 = v01 * v02 - v00 * v12
        c22 = v00 * v11 - v01 * v01
        inv = 1.0 / (v00 * c00 + v01 * c01 + v02 * c02)
        i00, i01, i02, i11, i12, i22 = [c * inv for c in (c00, c01, c02, c11, c12, c22)]
        vinv = ((i00, i01, i02), (i01, i11, i12), (i02, i12, i22))
        w = [dot3(vinv[a], s[6:9]) for a in range(3)]
        p = [[quantity(g, 24 + 3 * k + c) for c in range(3)] for k in range(2)]
        e = [quantity(g, 32 + k) for k in range(2)]
        use = [[dot3(vinv[a], p[k]) for a in range(3)] for k in range(2)]
        k00 = 1.0 - dot3(p[0], use[0])
        k01 = -dot3(p[0], use[1])
        k11 = 1.0 - dot3(p[1], use[1])
        sh = [e[k] - dot3(p[k], w) for k in range(2)]
        c0 = [quantity(g, c) for c in range(9)]
        c1 = [quantity(g, 9 + c) for c in range(9)]
        for c in range(9):
            red[c, at, :] = c0[c] * sh[0] + c1[c] * sh[1]
        base = (g % 2) * (8 * TS)
        for pos, (i, j) in enumerate(PAIRS):
            if j == 0:
                a0 = k00 * c0[i] + k01 * c1[i]
                a1 = k01 * c0[i] + k11 * c1[i]
            ts[pl.ds(base + pos, 8, stride=TS), :] = a0 * c0[j] + a1 * c1[j]
        for pos in range(45, 48):
            ts[pl.ds(base + pos, 8, stride=TS), :] = jnp.zeros((8, 128), F32)

        for j in range(8):
            x = ts[base + j * TS : base + j * TS + 48, :]
            odd = jnp.broadcast_to(slot_ref[g * 8 + j : g * 8 + j + 1, :] & 1, (48, 128)) == 1
            none = jnp.zeros((16, 128), F32)
            both = [jnp.where(odd, 0.0, x), none, jnp.where(odd, x, 0.0), none]
            x = jnp.transpose(jnp.concatenate(both, axis=0))
            hi = x.astype(BF16)
            rhs[g, j * 128 : j * 128 + 128, 0:128] = hi
            rhs[g, j * 128 : j * 128 + 128, 128:256] = (x - hi.astype(F32)).astype(BF16)

    def multiply(n, g):
        for k in (2 * n, 2 * n + 1):
            count = 32 // PARTS
            lhs = one_hot(slot_ref, g, 1, k * count, count)
            part = lax.dot_general(lhs, rhs[g], (((1,), (0,)), ((), ())), preferred_element_type=F32)
            at = pl.ds(k * 16 * count, 16 * count)
            acc[at, :] = part if g == 0 else acc[at, :] + part

    terms(0)
    for n in range(PARTS):
        for g in range(8):
            multiply(n, g)
            if n == 0 and g < 7:
                terms(g + 1)
            if g == 6 and n > 0:
                send(n - 1)
        done(n)


def one_hot(slot_ref, g, shift, start, groups, mask=63, upper=None):
    iota = lax.broadcasted_iota(I32, (16, 128), 0).astype(BF16)
    zero = jnp.zeros((16, 128), BF16)
    one = jnp.ones((16, 128), BF16)
    unit, group = [], []
    for j in range(8):
        slot = jnp.broadcast_to(slot_ref[pl.ds(g * 8 + j, 1), :], (16, 128))
        low = (slot >> shift) & 15
        if upper is not None:
            low = jnp.where((slot >> 10) == upper, low, 16)
        unit.append(jnp.where(low.astype(BF16) == iota, one, zero))
        group.append(((slot >> (shift + 4)) & mask).astype(BF16))
    rows = []
    for v in range(start, start + groups):
        mine = jnp.full((16, 128), v, BF16)
        rows.append(jnp.concatenate([jnp.where(group[j] == mine, unit[j], zero) for j in range(8)], axis=1))
    return jnp.concatenate(rows, axis=0)


def invert(owned, ent, inv_ref):
    lane = lax.broadcasted_iota(I32, (128, 128), 1)
    wide = jnp.concatenate([owned] * 16, axis=0)
    spread = lane_pick(jnp.transpose(wide), (lane & 15) >> 1)
    ent[...] = jnp.where(lane[0:64] & 1 == 0, spread[0:64], spread[64:128])
    entry = {pair: ent[pl.ds(pos, 8, stride=0), :] for pos, pair in enumerate(PAIRS)}
    factor, recip = {}, {}
    for c in range(9):
        r = lax.rsqrt(entry[c, c] + 1.0 if c == 0 else entry[c, c])
        recip[c] = r
        for i in range(c + 1, 9):
            factor[i, c] = entry[i, c] * r
        for i in range(c + 1, 9):
            for j in range(c + 1, i + 1):
                base = entry[i, j] + 1.0 if (i == j and c == 0) else entry[i, j]
                entry[i, j] = base - factor[i, c] * factor[j, c]
    solved = {}
    for c in range(9):
        solved[c, c] = recip[c]
        for i in range(c + 1, 9):
            value = factor[i, c] * solved[c, c]
            for k in range(c + 1, i):
                value = value + factor[i, k] * solved[k, c]
            solved[i, c] = -value * recip[i]
    row8 = lax.broadcasted_iota(I32, (8, 128), 0)
    lane8 = lax.broadcasted_iota(I32, (8, 128), 1)
    tile = jnp.zeros((8, 128), F32)
    for pos, (i, j) in enumerate(PAIRS):
        value = solved[i, i] * solved[i, j]
        for k in range(i + 1, 9):
            value = value + solved[k, i] * solved[k, j]
        inv_ref[9 * i + j : 9 * i + j + 1, :] = value[0:1, :]
        if i != j:
            inv_ref[9 * j + i : 9 * j + i + 1, :] = value[0:1, :]
        tile = jnp.where((row8 == pos % 8) & (lane8 // 16 == pos // 8), value, tile)
    return tile


def arrange(tiles, left):
    lane = lax.broadcasted_iota(I32, (8, 128), 1)
    for h in range(8):
        x = [tiles[h * 8 + e] for e in range(8)]
        for k in (1, 2, 4):
            upper = (lane // 16) & k != 0
            for e in range(8):
                if e & k == 0:
                    low, high = x[e], x[e + k]
                    x[e] = jnp.where(upper, pltpu.roll(high, 16 * k, 1), low)
                    x[e + k] = jnp.where(upper, high, pltpu.roll(low, 128 - 16 * k, 1))
        values = jnp.concatenate(x[0:6], axis=0)
        hi = values.astype(BF16)
        lo = (values - hi.astype(F32)).astype(BF16)
        at = pl.ds(128 * (h % 2), 128)
        left[96 * (h // 2) : 96 * (h // 2) + 48, at] = hi
        left[96 * (h // 2) + 48 : 96 * (h // 2) + 96, at] = lo


def choose(left, pick_ref, g, upper, store):
    chosen = lax.dot_general(
        left[...], one_hot(pick_ref, g, 0, 0, 16, 15, upper), (((1,), (0,)), ((), ())),
        preferred_element_type=F32,
    )
    for j in range(8):
        quarter = (jnp.broadcast_to(pick_ref[g * 8 + j : g * 8 + j + 1, :], (8, 128)) >> 8) & 3
        low, high = (quarter & 1) == 1, quarter > 1
        at = slice(128 * j, 128 * j + 128)
        for r in range(0, 48, 8):
            y = [chosen[96 * q + r : 96 * q + r + 8, at] + chosen[96 * q + 48 + r : 96 * q + 56 + r, at]
                 for q in range(4)]
            store(j, r, jnp.where(high, jnp.where(low, y[3], y[2]), jnp.where(low, y[1], y[0])))


def last(theirs, pick_ref, red_ref, rows_ref, near_ref, inv_ref, out_ref, left, picked, outs):
    arrange(theirs, left)
    inv_ref[...] = jnp.transpose(rows_ref[...])[0:16, 0:81]
    for g in range(8):
        base = (g % 2) * (8 * PS)

        def store(j, r, value):
            at = (g * 8 + j) * 48 + r
            picked[base + PS * j + r : base + PS * j + r + 8, :] = value + near_ref[at : at + 8, :]

        choose(left, pick_ref, g, 1, store)
        part = [red_ref[c, g * 8 : g * 8 + 8, :] for c in range(9)]
        total = [None] * 9
        for pos, (i, j) in enumerate(PAIRS):
            value = picked[pl.ds(base + pos, 8, stride=PS), :]
            for r, c in sorted({(i, j), (j, i)}):
                x = value * part[c]
                total[r] = x if total[r] is None else total[r] + x
        base = (g % 2) * (8 * OS)
        for r in range(9):
            outs[pl.ds(base + r, 8, stride=OS), :] = total[r]
        for j in range(8):
            at = pl.ds((g * 8 + j) * 128, 128)
            out_ref[0:8, at] = outs[base + j * OS : base + j * OS + 8, :]
            out_ref[8:9, at] = outs[base + j * OS + 8 : base + j * OS + 9, :]


def kernel(cam_hbm, pt_hbm, res_hbm, pid_hbm, cid_hbm, map_hbm, rank_hbm, theirs, pick_ref, red, rows_ref, near_ref,
           cam_ref, pt_ref, res_ref, pid_ref, cid_ref, map_ref, rank_ref, pos_ref,
           xs, ts, tot, heads, tails, fix, rhs, acc, ent,
           part, swap, half, recv, owned, mine, left, load_sems, swap_sems, send_sems, recv_sems):
    pts, core = lax.axis_index("pts"), lax.axis_index("grp")
    partner = (pts, 1 - core)
    chip_z = [(((pts >> 4) + d) & 3) << 4 for d in range(4)]
    chip_x = [(((pts >> 2) + d) & 3) << 2 for d in range(4)]
    chip_y = [(pts + d) & 3 for d in range(4)]

    def chip(off):
        return chip_z[off >> 4] + chip_x[(off >> 2) & 3] + chip_y[off & 3]

    pairs = [(cid_hbm, cid_ref), (map_hbm, map_ref), (rank_hbm, rank_ref), (pid_hbm, pid_ref),
             (pt_hbm, pt_ref), (res_hbm, res_ref), (cam_hbm, cam_ref)]
    loads = [pltpu.make_async_copy(src, dst, load_sems.at[n]) for n, (src, dst) in enumerate(pairs)]
    for load in loads:
        load.start()
    barrier = pltpu.get_barrier_semaphore()
    peers = [partner] + [(chip(off), core) for off in OFFSETS[:-1]]
    for peer in peers:
        pl.semaphore_signal(barrier, inc=1, device_id=peer, device_id_type=MESH)

    with jax.named_scope("load"):
        for load in loads[0:3]:
            load.wait()
    with jax.named_scope("slots"):
        find_slots(pts, core, cid_ref, map_ref, rank_ref, pos_ref, pick_ref)
        for load in loads[3:6]:
            load.wait()
        spread_points(pt_ref, res_ref, xs)

    def cameras_in():
        loads[6].wait()
        spread_cameras(cam_ref, xs)

    def swap_of(n):
        some = pl.ds(n * EACH, EACH)
        return pltpu.make_async_remote_copy(
            src_ref=part.at[some, 1 - core], dst_ref=swap.at[some], send_sem=swap_sems.at[n],
            recv_sem=swap_sems.at[PARTS + n], device_id=partner, device_id_type=MESH)

    def send(n):
        swap_of(n).wait()
        for r in range(n * EACH, n * EACH + EACH):
            half[r] = part[r, core] + swap[r]
        for r in range(n * EACH, n * EACH + EACH):
            if OFFSETS[r]:
                pltpu.make_async_remote_copy(
                    src_ref=half.at[r], dst_ref=recv.at[r], send_sem=send_sems.at[0],
                    recv_sem=recv_sems.at[0], device_id=(chip(OFFSETS[r]), core), device_id_type=MESH).start()

    def done(n):
        with jax.named_scope("send"):
            for r in range(n * EACH, n * EACH + EACH):
                at = pl.ds(r * 16, 16)
                part[r] = (acc[at, 0:128] + acc[at, 128:256]).reshape(2, 8, 128)
            if n == 0:
                pl.semaphore_wait(barrier, len(peers))
            swap_of(n).start()

    with jax.named_scope("points"):
        point_sums(pid_ref, xs, tot, heads, tails, fix, cameras_in)
    with jax.named_scope("cameras"):
        camera_sums(pid_ref, pos_ref, xs, tot, fix, red, ts, rhs, acc, done, send)
    with jax.named_scope("scatter"):
        send(PARTS - 1)
        pltpu.make_async_copy(recv, recv, recv_sems.at[0]).wait()

    with jax.named_scope("invert"):
        sums = [recv[n] for n in range(CHIPS - 1)] + [half[CHIPS - 1]]
        while len(sums) > 1:
            sums = [sums[i] + sums[i + 1] for i in range(0, len(sums), 2)]
        owned[...] = invert(sums[0], ent, rows_ref)
        mine[CHIPS - 1] = owned[...]

    with jax.named_scope("gather"):
        for off in OFFSETS[:-1]:
            pltpu.make_async_remote_copy(
                src_ref=owned, dst_ref=mine.at[RANK[back(off)]], send_sem=send_sems.at[1],
                recv_sem=recv_sems.at[1], device_id=(chip(off), core), device_id_type=MESH).start()
        pltpu.make_async_copy(recv, recv, recv_sems.at[1]).wait()
    with jax.named_scope("near"):
        across = pltpu.make_async_remote_copy(
            src_ref=mine, dst_ref=theirs, send_sem=swap_sems.at[0], recv_sem=swap_sems.at[PARTS],
            device_id=partner, device_id_type=MESH)
        across.start()
        arrange(mine, left)
        for g in range(8):
            def store(j, r, value):
                at = (g * 8 + j) * 48 + r
                near_ref[at : at + 8, :] = value

            choose(left, pick_ref, g, 0, store)
    with jax.named_scope("across"):
        pltpu.make_async_copy(recv, recv, send_sems.at[0]).wait()
        pltpu.make_async_copy(recv, recv, send_sems.at[1]).wait()
        across.wait()


def shards(cam_jac, pt_jac, resid, obs_point, obs_camera, camera_slot):
    vm = pltpu.VMEM
    dma = pltpu.SemaphoreType.DMA
    shape = jax.ShapeDtypeStruct
    ranks = np.zeros((8, 128), np.int32)
    ranks[:, OFFSETS] = np.arange(CHIPS)
    ranks = jnp.asarray(ranks)
    theirs, picks, red, rows, near = pl.pallas_call(
        kernel,
        out_shape=(
            shape((CHIPS, 8, 128), F32),
            shape((64, 128), I32),
            shape((9, 64, 128), F32),
            shape((128, 128), F32),
            shape((64 * 48, 128), F32),
        ),
        in_specs=[pl.BlockSpec(memory_space=pltpu.HBM)] * 7,
        out_specs=[pl.BlockSpec(memory_space=vm)] * 5,
        scratch_shapes=[
            vm((18, 8192), F32),
            vm((6, 8192), F32),
            vm((2, 8192), F32),
            vm((64, 128), I32),
            vm((64, 128), I32),
            vm((16, 128), I32),
            vm((8, 128), I32),
            vm((64, 128), I32),
            vm((64 * XS, 128), F32),
            vm((16 * TS, 128), F32),
            vm((9 * 64, 128), F32),
            vm((64, 128), F32),
            vm((64, 128), F32),
            vm((128, 128), F32),
            vm((8, 1024, 256), BF16),
            vm((1024, 256), F32),
            vm((64, 128), F32),
            vm((CHIPS, 2, 8, 128), F32),
            vm((CHIPS, 8, 128), F32),
            vm((CHIPS, 8, 128), F32),
            vm((CHIPS - 1, 8, 128), F32),
            vm((8, 128), F32),
            vm((CHIPS, 8, 128), F32),
            vm((384, 256), BF16),
            dma((7,)),
            dma((2 * PARTS,)),
            dma((2,)),
            dma((6,)),
        ],
        compiler_params=pltpu.CompilerParams(
            vmem_limit_bytes=28 * 2**20, collective_id=0, has_side_effects=True
        ),
        name="schur",
    )(
        *[
            pltpu.with_memory_space_constraint(x, pltpu.HBM)
            for x in (
                cam_jac,
                pt_jac,
                resid,
                obs_point.reshape(64, 128),
                obs_camera.reshape(64, 128),
                camera_slot.reshape(16, 128),
                ranks,
            )
        ]
    )
    inverse, precond = pl.pallas_call(
        last,
        out_shape=(shape((16, 81), F32), shape((9, 8192), F32)),
        in_specs=[pl.BlockSpec(memory_space=vm)] * 5,
        out_specs=[pl.BlockSpec(memory_space=vm)] * 2,
        scratch_shapes=[
            vm((384, 256), BF16),
            vm((16 * PS, 128), F32),
            vm((16 * OS, 128), F32),
        ],
        compiler_params=pltpu.CompilerParams(vmem_limit_bytes=28 * 2**20),
        name="last",
    )(theirs, picks, red, rows, near)
    return inverse.T, precond


def solution(mesh):
    both = ("pts", "grp")
    in_specs = (P(None, both), P(None, both), P(None, both), P(both), P(both), P())
    out_specs = (P(None, both), P(None, both))
    return jax.shard_map(shards, mesh=mesh, in_specs=in_specs, out_specs=out_specs, check_vma=False)
```

```python
import jax
import jax.numpy as jnp
import numpy as np
from jax import lax
from jax.experimental import pallas as pl
from jax.experimental.pallas import tpu as pltpu
from jax.sharding import PartitionSpec as P

F32, BF16, I32 = jnp.float32, jnp.bfloat16, jnp.int32
MESH = pl.DeviceIdType.MESH
XS = 40
TS = 56
OS = 24
PS = 56
PAIRS = [(i, j) for i in range(9) for j in range(i + 1)]
CHIPS = 64


def hops(off):
    return sum(min(d, 4 - d) for d in (off // 16, off // 4 % 4, off % 4))


OFFSETS = sorted(range(CHIPS), key=lambda off: (-hops(off), off))
RANK = {off: r for r, off in enumerate(OFFSETS)}
PARTS = 4
EACH = CHIPS // PARTS
AHEAD = 5
CLOSE = 3 * EACH


def back(off):
    return ((-(off >> 4) & 3) << 4) | ((-(off >> 2) & 3) << 2) | (-off & 3)


def m8(x):
    return pl.multiple_of(x, 8)


def lane_pick(row, idx):
    return jnp.take_along_axis(row, idx, axis=1, mode="promise_in_bounds")


def find_slots(pts, core, cid_ref, map_ref, rank_ref, pos_ref, pick_ref):
    z, x, y = pts >> 4, (pts >> 2) & 3, pts & 3
    rank = rank_ref[...]
    for g in range(8):
        cid = cid_ref[g * 8 : g * 8 + 8, :]
        lo = cid & 127
        vals = [lane_pick(map_ref[pl.ds(h, 8, stride=0), :], lo) for h in range(16)]
        for b in range(4):
            bit = ((cid >> (7 + b)) & 1) == 1
            vals = [jnp.where(bit, vals[2 * i + 1], vals[2 * i]) for i in range(len(vals) // 2)]
        slot = vals[0]
        off = ((((slot >> 9) - z) & 3) << 4) | ((((slot >> 7) - x) & 3) << 2) | (((slot >> 5) - y) & 3)
        near = lane_pick(rank, off)
        pos_ref[g * 8 : g * 8 + 8, :] = (near << 5) | (slot & 31)
        pick_ref[g * 8 : g * 8 + 8, :] = ((((slot >> 4) & 1) ^ core) << 10) | (near << 4) | (slot & 15)


def spread_points(pt_ref, res_ref, xs):
    for j in range(64):
        at = pl.ds(j * 128, 128)
        xs[j * XS + 24 : j * XS + 30, :] = pt_ref[0:6, at]
        xs[j * XS + 32 : j * XS + 34, :] = res_ref[0:2, at]


def spread_cameras(cam_ref, xs):
    for j in range(64):
        at = pl.ds(j * 128, 128)
        xs[j * XS : j * XS + 8, :] = cam_ref[0:8, at]
        xs[j * XS + 8 : j * XS + 16, :] = cam_ref[8:16, at]
        xs[j * XS + 16 : j * XS + 18, :] = cam_ref[16:18, at]


def point_sums(pid_ref, xs, tot, heads, tails, fix, between):
    lane = lax.broadcasted_iota(I32, (8, 128), 1)

    def quantity(g, q):
        return xs[pl.ds(g * (8 * XS) + q, 8, stride=XS), :]

    def one(g):
        p = [[quantity(g, 24 + 3 * k + c) for c in range(3)] for k in range(2)]
        e = [quantity(g, 32 + k) for k in range(2)]
        pid = pid_ref[pl.ds(m8(g * 8), 8), :]
        v = [p[0][a] * p[0][c] + p[1][a] * p[1][c] for a in range(3) for c in range(a, 3)]
        v += [p[0][a] * e[0] + p[1][a] * e[1] for a in range(3)]
        return pid, v, lane

    def scan(state, k):
        pid, v, end = state
        same = (pltpu.roll(pid, k, 1) == pid) & (lane >= k)
        v = [x + jnp.where(same, pltpu.roll(x, k, 1), 0.0) for x in v]
        after = (pltpu.roll(pid, 128 - k, 1) == pid) & (lane < 128 - k)
        return pid, v, jnp.where(after, pltpu.roll(end, 128 - k, 1), end)

    def finish(g, state):
        pid, v, end = state
        head = jnp.zeros((8, 128), F32)
        tail = jnp.zeros((8, 128), F32)
        for q in range(9):
            full = lane_pick(v[q], end)
            tot[pl.ds(m8(q * 64 + g * 8), 8), :] = full
            ends = pltpu.roll(full, q + 1, 1)
            head = jnp.where(lane == q + 1, ends, head)
            tail = jnp.where(lane == q, ends, tail)
        heads[pl.ds(m8(g * 8), 8), :] = head
        tails[pl.ds(m8(g * 8), 8), :] = tail

    def step(n, carry):
        states = [one(n * 4 + u) for u in range(4)]
        for b in range(7):
            states = [scan(state, 1 << b) for state in states]
        for u in range(4):
            finish(n * 4 + u, states[u])
        return carry

    lax.fori_loop(0, 2, step, 0)
    between()

    pid = pid_ref[...]
    first = jnp.broadcast_to(pid[:, 0:1], (64, 128))
    last = jnp.broadcast_to(pid[:, 127:128], (64, 128))
    ends = jnp.where(lax.broadcasted_iota(I32, (64, 128), 1) < 64, first, last).astype(F32)
    across = jnp.transpose(ends)
    r0 = lax.broadcasted_iota(I32, (64, 64), 0)
    r1 = lax.broadcasted_iota(I32, (64, 64), 1)
    from_before = (r1 < r0) & (across[64:128, :] == first[:, 0:64].astype(F32))
    from_after = (r1 > r0) & (across[0:64, :] == last[:, 0:64].astype(F32))

    def total(which, values):
        return lax.dot_general(
            jnp.where(which, 1.0, 0.0),
            values[...],
            (((1,), (0,)), ((), ())),
            precision=lax.Precision.HIGHEST,
            preferred_element_type=F32,
        )

    fix[0:64, :] = total(from_before, tails)
    fix[64:128, :] = total(from_after, heads)


def camera_sums(pid_ref, slot_ref, xs, tot, fix, red, ts, rhs, acc, done, send):
    def quantity(g, q):
        return xs[pl.ds(g * (8 * XS) + q, 8, stride=XS), :]

    def dot3(a, b):
        return a[0] * b[0] + a[1] * b[1] + a[2] * b[2]

    def terms(g):
        at = pl.ds(g * 8, 8)
        pid = pid_ref[at, :]
        pre = fix[at, :]
        post = fix[pl.ds(64 + g * 8, 8), :]
        is_first = pid == jnp.broadcast_to(pid[:, 0:1], (8, 128))
        is_last = pid == jnp.broadcast_to(pid[:, 127:128], (8, 128))
        s = []
        for q in range(9):
            x = tot[pl.ds(q * 64 + g * 8, 8), :]
            x = x + jnp.where(is_first, jnp.broadcast_to(pre[:, q : q + 1], (8, 128)), 0.0)
            x = x + jnp.where(is_last, jnp.broadcast_to(post[:, q + 1 : q + 2], (8, 128)), 0.0)
            s.append(x)
        v00, v01, v02, v11, v12, v22 = s[0] + 1.0, s[1], s[2], s[3] + 1.0, s[4], s[5] + 1.0
        c00 = v11 * v22 - v12 * v12
        c01 = v02 * v12 - v01 * v22
        c02 = v01 * v12 - v02 * v11
        c11 = v00 * v22 - v02 * v02
        c12 = v01 * v02 - v00 * v12
        c22 = v00 * v11 - v01 * v01
        inv = 1.0 / (v00 * c00 + v01 * c01 + v02 * c02)
        i00, i01, i02, i11, i12, i22 = [c * inv for c in (c00, c01, c02, c11, c12, c22)]
        vinv = ((i00, i01, i02), (i01, i11, i12), (i02, i12, i22))
        w = [dot3(vinv[a], s[6:9]) for a in range(3)]
        p = [[quantity(g, 24 + 3 * k + c) for c in range(3)] for k in range(2)]
        e = [quantity(g, 32 + k) for k in range(2)]
        use = [[dot3(vinv[a], p[k]) for a in range(3)] for k in range(2)]
        k00 = 1.0 - dot3(p[0], use[0])
        k01 = -dot3(p[0], use[1])
        k11 = 1.0 - dot3(p[1], use[1])
        sh = [e[k] - dot3(p[k], w) for k in range(2)]
        c0 = [quantity(g, c) for c in range(9)]
        c1 = [quantity(g, 9 + c) for c in range(9)]
        for c in range(9):
            red[c, at, :] = c0[c] * sh[0] + c1[c] * sh[1]
        base = (g % 2) * (8 * TS)
        for pos, (i, j) in enumerate(PAIRS):
            if j == 0:
                a0 = k00 * c0[i] + k01 * c1[i]
                a1 = k01 * c0[i] + k11 * c1[i]
            ts[pl.ds(base + pos, 8, stride=TS), :] = a0 * c0[j] + a1 * c1[j]
        for pos in range(45, 48):
            ts[pl.ds(base + pos, 8, stride=TS), :] = jnp.zeros((8, 128), F32)

        for j in range(8):
            x = ts[base + j * TS : base + j * TS + 48, :]
            odd = jnp.broadcast_to(slot_ref[g * 8 + j : g * 8 + j + 1, :] & 1, (48, 128)) == 1
            none = jnp.zeros((16, 128), F32)
            both = [jnp.where(odd, 0.0, x), none, jnp.where(odd, x, 0.0), none]
            x = jnp.transpose(jnp.concatenate(both, axis=0))
            hi = x.astype(BF16)
            rhs[g, j * 128 : j * 128 + 128, 0:128] = hi
            rhs[g, j * 128 : j * 128 + 128, 128:256] = (x - hi.astype(F32)).astype(BF16)

    def multiply(n, g):
        for k in (2 * n, 2 * n + 1):
            count = 32 // PARTS
            lhs = one_hot(slot_ref, g, 1, k * count, count)
            part = lax.dot_general(lhs, rhs[g], (((1,), (0,)), ((), ())), preferred_element_type=F32)
            at = pl.ds(k * 16 * count, 16 * count)
            acc[at, :] = part if g == 0 else acc[at, :] + part

    terms(0)
    for g in range(8):
        multiply(0, g)
        if g < AHEAD:
            multiply(1, g)
        if g < 7:
            terms(g + 1)
    done(0)
    for g in range(AHEAD, 8):
        multiply(1, g)
    done(1)
    for g in range(8):
        multiply(2, g)
        if g == 3:
            send(0)
    done(2)
    for g in range(8):
        multiply(3, g)
        if g == 0:
            send(1)
        if g == 6:
            send(2)
    done(3)


def one_hot(slot_ref, g, shift, start, groups, mask=63, upper=None):
    iota = lax.broadcasted_iota(I32, (16, 128), 0).astype(BF16)
    zero = jnp.zeros((16, 128), BF16)
    one = jnp.ones((16, 128), BF16)
    unit, group = [], []
    for j in range(8):
        slot = jnp.broadcast_to(slot_ref[pl.ds(g * 8 + j, 1), :], (16, 128))
        low = (slot >> shift) & 15
        if upper is not None:
            low = jnp.where((slot >> 10) == upper, low, 16)
        unit.append(jnp.where(low.astype(BF16) == iota, one, zero))
        group.append(((slot >> (shift + 4)) & mask).astype(BF16))
    rows = []
    for v in range(start, start + groups):
        mine = jnp.full((16, 128), v, BF16)
        rows.append(jnp.concatenate([jnp.where(group[j] == mine, unit[j], zero) for j in range(8)], axis=1))
    return jnp.concatenate(rows, axis=0)


def invert(owned, ent, inv_ref):
    lane = lax.broadcasted_iota(I32, (128, 128), 1)
    wide = jnp.concatenate([owned] * 16, axis=0)
    spread = lane_pick(jnp.transpose(wide), (lane & 15) >> 1)
    ent[...] = jnp.where(lane[0:64] & 1 == 0, spread[0:64], spread[64:128])
    entry = {pair: ent[pl.ds(pos, 8, stride=0), :] for pos, pair in enumerate(PAIRS)}
    factor, recip = {}, {}
    for c in range(9):
        r = lax.rsqrt(entry[c, c] + 1.0 if c == 0 else entry[c, c])
        recip[c] = r
        for i in range(c + 1, 9):
            factor[i, c] = entry[i, c] * r
        for i in range(c + 1, 9):
            for j in range(c + 1, i + 1):
                base = entry[i, j] + 1.0 if (i == j and c == 0) else entry[i, j]
                entry[i, j] = base - factor[i, c] * factor[j, c]
    solved = {}
    for c in range(9):
        solved[c, c] = recip[c]
        for i in range(c + 1, 9):
            value = factor[i, c] * solved[c, c]
            for k in range(c + 1, i):
                value = value + factor[i, k] * solved[k, c]
            solved[i, c] = -value * recip[i]
    row8 = lax.broadcasted_iota(I32, (8, 128), 0)
    lane8 = lax.broadcasted_iota(I32, (8, 128), 1)
    tile = jnp.zeros((8, 128), F32)
    for pos, (i, j) in enumerate(PAIRS):
        value = solved[i, i] * solved[i, j]
        for k in range(i + 1, 9):
            value = value + solved[k, i] * solved[k, j]
        inv_ref[9 * i + j : 9 * i + j + 1, :] = value[0:1, :]
        if i != j:
            inv_ref[9 * j + i : 9 * j + i + 1, :] = value[0:1, :]
        tile = jnp.where((row8 == pos % 8) & (lane8 // 16 == pos // 8), value, tile)
    return tile


def arrange(tiles, left):
    lane = lax.broadcasted_iota(I32, (8, 128), 1)
    for h in range(8):
        x = [tiles[h * 8 + e] for e in range(8)]
        for k in (1, 2, 4):
            upper = (lane // 16) & k != 0
            for e in range(8):
                if e & k == 0:
                    low, high = x[e], x[e + k]
                    x[e] = jnp.where(upper, pltpu.roll(high, 16 * k, 1), low)
                    x[e + k] = jnp.where(upper, high, pltpu.roll(low, 128 - 16 * k, 1))
        values = jnp.concatenate(x[0:6], axis=0)
        hi = values.astype(BF16)
        lo = (values - hi.astype(F32)).astype(BF16)
        at = pl.ds(128 * (h % 2), 128)
        left[96 * (h // 2) : 96 * (h // 2) + 48, at] = hi
        left[96 * (h // 2) + 48 : 96 * (h // 2) + 96, at] = lo


def choose(left, pick_ref, g, upper, store):
    chosen = lax.dot_general(
        left[...], one_hot(pick_ref, g, 0, 0, 16, 15, upper), (((1,), (0,)), ((), ())),
        preferred_element_type=F32,
    )
    for j in range(8):
        quarter = (jnp.broadcast_to(pick_ref[g * 8 + j : g * 8 + j + 1, :], (8, 128)) >> 8) & 3
        low, high = (quarter & 1) == 1, quarter > 1
        at = slice(128 * j, 128 * j + 128)
        for r in range(0, 48, 8):
            y = [chosen[96 * q + r : 96 * q + r + 8, at] + chosen[96 * q + 48 + r : 96 * q + 56 + r, at]
                 for q in range(4)]
            store(j, r, jnp.where(high, jnp.where(low, y[3], y[2]), jnp.where(low, y[1], y[0])))


def last(theirs, pick_ref, red_ref, rows_ref, near_ref, inv_ref, out_ref, left, picked, outs):
    arrange(theirs, left)
    inv_ref[...] = jnp.transpose(rows_ref[...])[0:16, 0:81]
    for g in range(8):
        base = (g % 2) * (8 * PS)

        def store(j, r, value):
            at = (g * 8 + j) * 48 + r
            picked[base + PS * j + r : base + PS * j + r + 8, :] = value + near_ref[at : at + 8, :]

        choose(left, pick_ref, g, 1, store)
        part = [red_ref[c, g * 8 : g * 8 + 8, :] for c in range(9)]
        total = [None] * 9
        for pos, (i, j) in enumerate(PAIRS):
            value = picked[pl.ds(base + pos, 8, stride=PS), :]
            for r, c in sorted({(i, j), (j, i)}):
                x = value * part[c]
                total[r] = x if total[r] is None else total[r] + x
        base = (g % 2) * (8 * OS)
        for r in range(9):
            outs[pl.ds(base + r, 8, stride=OS), :] = total[r]
        for j in range(8):
            at = pl.ds((g * 8 + j) * 128, 128)
            out_ref[0:8, at] = outs[base + j * OS : base + j * OS + 8, :]
            out_ref[8:9, at] = outs[base + j * OS + 8 : base + j * OS + 9, :]


def kernel(cam_hbm, pt_hbm, res_hbm, pid_hbm, cid_hbm, map_hbm, rank_hbm, theirs, pick_ref, red, rows_ref, near_ref,
           cam_ref, pt_ref, res_ref, pid_ref, cid_ref, map_ref, rank_ref, pos_ref,
           xs, ts, tot, heads, tails, fix, rhs, acc, ent,
           part, swap, half, recv, owned, mine, left, load_sems, swap_sems, send_sems, recv_sems):
    pts, core = lax.axis_index("pts"), lax.axis_index("grp")
    partner = (pts, 1 - core)
    chip_z = [(((pts >> 4) + d) & 3) << 4 for d in range(4)]
    chip_x = [(((pts >> 2) + d) & 3) << 2 for d in range(4)]
    chip_y = [(pts + d) & 3 for d in range(4)]

    def chip(off):
        return chip_z[off >> 4] + chip_x[(off >> 2) & 3] + chip_y[off & 3]

    pairs = [(pt_hbm, pt_ref), (res_hbm, res_ref), (pid_hbm, pid_ref), (cid_hbm, cid_ref),
             (map_hbm, map_ref), (rank_hbm, rank_ref), (cam_hbm, cam_ref)]
    loads = [pltpu.make_async_copy(src, dst, load_sems.at[n]) for n, (src, dst) in enumerate(pairs)]
    for load in loads:
        load.start()
    barrier = pltpu.get_barrier_semaphore()
    peers = [partner] + [(chip(off), core) for off in OFFSETS[:-1]]
    peers += [(chip(off), 1 - core) for off in OFFSETS[:-1] if off in OFFSETS[CLOSE:] or back(off) in OFFSETS[CLOSE:]]
    for peer in peers:
        pl.semaphore_signal(barrier, inc=1, device_id=peer, device_id_type=MESH)

    with jax.named_scope("load"):
        for load in loads[0:3]:
            load.wait()
        spread_points(pt_ref, res_ref, xs)

    def cameras_in():
        for load in loads[3:]:
            load.wait()
        find_slots(pts, core, cid_ref, map_ref, rank_ref, pos_ref, pick_ref)
        spread_cameras(cam_ref, xs)

    def swap_of(n):
        some = pl.ds(n * EACH, EACH)
        return pltpu.make_async_remote_copy(
            src_ref=part.at[some, 1 - core], dst_ref=swap.at[some], send_sem=swap_sems.at[n],
            recv_sem=swap_sems.at[PARTS + n], device_id=partner, device_id_type=MESH)

    def give(src, slot, device):
        pltpu.make_async_remote_copy(
            src_ref=src, dst_ref=recv.at[slot], send_sem=send_sems.at[0], recv_sem=recv_sems.at[0],
            device_id=device, device_id_type=MESH).start()

    def send(n):
        swap_of(n).wait()
        for r in range(n * EACH, n * EACH + EACH):
            half[r] = part[r, core] + swap[r]
        for r in range(n * EACH, n * EACH + EACH):
            give(half.at[r], r, (chip(OFFSETS[r]), core))

    def done(n):
        with jax.named_scope("send"):
            for r in range(n * EACH, n * EACH + EACH):
                at = pl.ds(r * 16, 16)
                part[r] = (acc[at, 0:128] + acc[at, 128:256]).reshape(2, 8, 128)
            if n == 0:
                pl.semaphore_wait(barrier, len(peers))
            if n < PARTS - 1:
                swap_of(n).start()
            else:
                for r in range(CLOSE, CHIPS):
                    to = chip(OFFSETS[r])
                    if r < CHIPS - 1:
                        give(part.at[r, core], r, (to, core))
                    give(part.at[r, 1 - core], CHIPS - 1 + r - CLOSE, (to, 1 - core))

    with jax.named_scope("points"):
        point_sums(pid_ref, xs, tot, heads, tails, fix, cameras_in)
    with jax.named_scope("cameras"):
        camera_sums(pid_ref, pos_ref, xs, tot, fix, red, ts, rhs, acc, done, send)
    with jax.named_scope("scatter"):
        pltpu.make_async_copy(recv, recv, recv_sems.at[0]).wait()

    with jax.named_scope("invert"):
        sums = [recv[n] for n in range(CHIPS - 1 + EACH)] + [part[CHIPS - 1, core]]
        while len(sums) > 1:
            sums = [sums[i] + sums[i + 1] for i in range(0, len(sums) - 1, 2)] + sums[len(sums) & ~1 :]
        owned[...] = invert(sums[0], ent, rows_ref)
        mine[CHIPS - 1] = owned[...]

    with jax.named_scope("gather"):
        for off in OFFSETS[:-1]:
            pltpu.make_async_remote_copy(
                src_ref=owned, dst_ref=mine.at[RANK[back(off)]], send_sem=send_sems.at[1],
                recv_sem=recv_sems.at[1], device_id=(chip(off), core), device_id_type=MESH).start()
        others = recv.at[0 : CHIPS - 1]
        pltpu.make_async_copy(others, others, recv_sems.at[1]).wait()
    with jax.named_scope("near"):
        across = pltpu.make_async_remote_copy(
            src_ref=mine, dst_ref=theirs, send_sem=swap_sems.at[0], recv_sem=swap_sems.at[PARTS],
            device_id=partner, device_id_type=MESH)
        across.start()
        arrange(mine, left)
        for g in range(8):
            def store(j, r, value):
                at = (g * 8 + j) * 48 + r
                near_ref[at : at + 8, :] = value

            choose(left, pick_ref, g, 0, store)
    with jax.named_scope("across"):
        pltpu.make_async_copy(recv, recv, send_sems.at[0]).wait()
        pltpu.make_async_copy(others, others, send_sems.at[1]).wait()
        across.wait()


def shards(cam_jac, pt_jac, resid, obs_point, obs_camera, camera_slot):
    vm = pltpu.VMEM
    dma = pltpu.SemaphoreType.DMA
    shape = jax.ShapeDtypeStruct
    ranks = np.zeros((8, 128), np.int32)
    ranks[:, OFFSETS] = np.arange(CHIPS)
    ranks = jnp.asarray(ranks)
    theirs, picks, red, rows, near = pl.pallas_call(
        kernel,
        out_shape=(
            shape((CHIPS, 8, 128), F32),
            shape((64, 128), I32),
            shape((9, 64, 128), F32),
            shape((128, 128), F32),
            shape((64 * 48, 128), F32),
        ),
        in_specs=[pl.BlockSpec(memory_space=pltpu.HBM)] * 7,
        out_specs=[pl.BlockSpec(memory_space=vm)] * 5,
        scratch_shapes=[
            vm((18, 8192), F32),
            vm((6, 8192), F32),
            vm((2, 8192), F32),
            vm((64, 128), I32),
            vm((64, 128), I32),
            vm((16, 128), I32),
            vm((8, 128), I32),
            vm((64, 128), I32),
            vm((64 * XS, 128), F32),
            vm((16 * TS, 128), F32),
            vm((9 * 64, 128), F32),
            vm((64, 128), F32),
            vm((64, 128), F32),
            vm((128, 128), F32),
            vm((8, 1024, 256), BF16),
            vm((1024, 256), F32),
            vm((64, 128), F32),
            vm((CHIPS, 2, 8, 128), F32),
            vm((CLOSE, 8, 128), F32),
            vm((CLOSE, 8, 128), F32),
            vm((CHIPS - 1 + EACH, 8, 128), F32),
            vm((8, 128), F32),
            vm((CHIPS, 8, 128), F32),
            vm((384, 256), BF16),
            dma((7,)),
            dma((2 * PARTS,)),
            dma((2,)),
            dma((6,)),
        ],
        compiler_params=pltpu.CompilerParams(
            vmem_limit_bytes=28 * 2**20, collective_id=0, has_side_effects=True
        ),
        name="schur",
    )(
        *[
            pltpu.with_memory_space_constraint(x, pltpu.HBM)
            for x in (
                cam_jac,
                pt_jac,
                resid,
                obs_point.reshape(64, 128),
                obs_camera.reshape(64, 128),
                camera_slot.reshape(16, 128),
                ranks,
            )
        ]
    )
    inverse, precond = pl.pallas_call(
        last,
        out_shape=(shape((16, 81), F32), shape((9, 8192), F32)),
        in_specs=[pl.BlockSpec(memory_space=vm)] * 5,
        out_specs=[pl.BlockSpec(memory_space=vm)] * 2,
        scratch_shapes=[
            vm((384, 256), BF16),
            vm((16 * PS, 128), F32),
            vm((16 * OS, 128), F32),
        ],
        compiler_params=pltpu.CompilerParams(vmem_limit_bytes=28 * 2**20),
        name="last",
    )(theirs, picks, red, rows, near)
    return inverse.T, precond


def solution(mesh):
    both = ("pts", "grp")
    in_specs = (P(None, both), P(None, both), P(None, both), P(both), P(both), P())
    out_specs = (P(None, both), P(None, both))
    return jax.shard_map(shards, mesh=mesh, in_specs=in_specs, out_specs=out_specs, check_vma=False)
```

```python
import jax
import jax.numpy as jnp
import numpy as np
from jax import lax
from jax.experimental import pallas as pl
from jax.experimental.pallas import tpu as pltpu
from jax.sharding import PartitionSpec as P

F32, BF16, I32 = jnp.float32, jnp.bfloat16, jnp.int32
MESH = pl.DeviceIdType.MESH
XS = 40
TS = 56
OS = 24
PS = 56
PAIRS = [(i, j) for i in range(9) for j in range(i + 1)]
CHIPS = 64


def hops(off):
    return sum(min(d, 4 - d) for d in (off // 16, off // 4 % 4, off % 4))


OFFSETS = sorted(range(CHIPS), key=lambda off: (-hops(off), off))
RANK = {off: r for r, off in enumerate(OFFSETS)}
PARTS = 4
EACH = CHIPS // PARTS
AHEAD = 5
CLOSE = 3 * EACH


def back(off):
    return ((-(off >> 4) & 3) << 4) | ((-(off >> 2) & 3) << 2) | (-off & 3)


def m8(x):
    return pl.multiple_of(x, 8)


def lane_pick(row, idx):
    return jnp.take_along_axis(row, idx, axis=1, mode="promise_in_bounds")


def find_slots(pts, core, cid_ref, map_ref, rank_ref, pos_ref, pick_ref):
    z, x, y = pts >> 4, (pts >> 2) & 3, pts & 3
    rank = rank_ref[...]
    for g in range(8):
        cid = cid_ref[g * 8 : g * 8 + 8, :]
        lo = cid & 127
        vals = [lane_pick(map_ref[pl.ds(h, 8, stride=0), :], lo) for h in range(16)]
        for b in range(4):
            bit = ((cid >> (7 + b)) & 1) == 1
            vals = [jnp.where(bit, vals[2 * i + 1], vals[2 * i]) for i in range(len(vals) // 2)]
        slot = vals[0]
        off = ((((slot >> 9) - z) & 3) << 4) | ((((slot >> 7) - x) & 3) << 2) | (((slot >> 5) - y) & 3)
        near = lane_pick(rank, off)
        pos_ref[g * 8 : g * 8 + 8, :] = (near << 5) | (slot & 31)
        pick_ref[g * 8 : g * 8 + 8, :] = ((((slot >> 4) & 1) ^ core) << 10) | (near << 4) | (slot & 15)


def spread_points(pt_ref, res_ref, xs):
    for j in range(64):
        at = pl.ds(j * 128, 128)
        xs[j * XS + 24 : j * XS + 30, :] = pt_ref[0:6, at]
        xs[j * XS + 32 : j * XS + 34, :] = res_ref[0:2, at]


def spread_cameras(cam_ref, xs):
    for j in range(64):
        at = pl.ds(j * 128, 128)
        xs[j * XS : j * XS + 8, :] = cam_ref[0:8, at]
        xs[j * XS + 8 : j * XS + 16, :] = cam_ref[8:16, at]
        xs[j * XS + 16 : j * XS + 18, :] = cam_ref[16:18, at]


def point_sums(pid_ref, xs, tot, heads, tails, fix, between):
    lane = lax.broadcasted_iota(I32, (8, 128), 1)

    def quantity(g, q):
        return xs[pl.ds(g * (8 * XS) + q, 8, stride=XS), :]

    def one(g):
        p = [[quantity(g, 24 + 3 * k + c) for c in range(3)] for k in range(2)]
        e = [quantity(g, 32 + k) for k in range(2)]
        pid = pid_ref[pl.ds(m8(g * 8), 8), :]
        v = [p[0][a] * p[0][c] + p[1][a] * p[1][c] for a in range(3) for c in range(a, 3)]
        v += [p[0][a] * e[0] + p[1][a] * e[1] for a in range(3)]
        return pid, v, lane

    def scan(state, k):
        pid, v, end = state
        same = (pltpu.roll(pid, k, 1) == pid) & (lane >= k)
        v = [x + jnp.where(same, pltpu.roll(x, k, 1), 0.0) for x in v]
        after = (pltpu.roll(pid, 128 - k, 1) == pid) & (lane < 128 - k)
        return pid, v, jnp.where(after, pltpu.roll(end, 128 - k, 1), end)

    def finish(g, state):
        pid, v, end = state
        head = jnp.zeros((8, 128), F32)
        tail = jnp.zeros((8, 128), F32)
        for q in range(9):
            full = lane_pick(v[q], end)
            tot[pl.ds(m8(q * 64 + g * 8), 8), :] = full
            ends = pltpu.roll(full, q + 1, 1)
            head = jnp.where(lane == q + 1, ends, head)
            tail = jnp.where(lane == q, ends, tail)
        heads[pl.ds(m8(g * 8), 8), :] = head
        tails[pl.ds(m8(g * 8), 8), :] = tail

    states = [one(g) for g in range(8)]
    for b in range(7):
        states = [scan(state, 1 << b) for state in states]
    for g in range(8):
        finish(g, states[g])
    between()

    pid = pid_ref[...]
    first = jnp.broadcast_to(pid[:, 0:1], (64, 128))
    last = jnp.broadcast_to(pid[:, 127:128], (64, 128))
    ends = jnp.where(lax.broadcasted_iota(I32, (64, 128), 1) < 64, first, last).astype(F32)
    across = jnp.transpose(ends)
    r0 = lax.broadcasted_iota(I32, (64, 64), 0)
    r1 = lax.broadcasted_iota(I32, (64, 64), 1)
    from_before = (r1 < r0) & (across[64:128, :] == first[:, 0:64].astype(F32))
    from_after = (r1 > r0) & (across[0:64, :] == last[:, 0:64].astype(F32))

    def total(which, values):
        return lax.dot_general(
            jnp.where(which, 1.0, 0.0),
            values[...],
            (((1,), (0,)), ((), ())),
            precision=lax.Precision.HIGHEST,
            preferred_element_type=F32,
        )

    fix[0:64, :] = total(from_before, tails)
    fix[64:128, :] = total(from_after, heads)


def camera_sums(pid_ref, slot_ref, xs, tot, fix, red, ts, rhs, acc, done, send):
    def quantity(g, q):
        return xs[pl.ds(g * (8 * XS) + q, 8, stride=XS), :]

    def dot3(a, b):
        return a[0] * b[0] + a[1] * b[1] + a[2] * b[2]

    def terms(g):
        at = pl.ds(g * 8, 8)
        pid = pid_ref[at, :]
        pre = fix[at, :]
        post = fix[pl.ds(64 + g * 8, 8), :]
        is_first = pid == jnp.broadcast_to(pid[:, 0:1], (8, 128))
        is_last = pid == jnp.broadcast_to(pid[:, 127:128], (8, 128))
        s = []
        for q in range(9):
            x = tot[pl.ds(q * 64 + g * 8, 8), :]
            x = x + jnp.where(is_first, jnp.broadcast_to(pre[:, q : q + 1], (8, 128)), 0.0)
            x = x + jnp.where(is_last, jnp.broadcast_to(post[:, q + 1 : q + 2], (8, 128)), 0.0)
            s.append(x)
        v00, v01, v02, v11, v12, v22 = s[0] + 1.0, s[1], s[2], s[3] + 1.0, s[4], s[5] + 1.0
        c00 = v11 * v22 - v12 * v12
        c01 = v02 * v12 - v01 * v22
        c02 = v01 * v12 - v02 * v11
        c11 = v00 * v22 - v02 * v02
        c12 = v01 * v02 - v00 * v12
        c22 = v00 * v11 - v01 * v01
        inv = 1.0 / (v00 * c00 + v01 * c01 + v02 * c02)
        i00, i01, i02, i11, i12, i22 = [c * inv for c in (c00, c01, c02, c11, c12, c22)]
        vinv = ((i00, i01, i02), (i01, i11, i12), (i02, i12, i22))
        w = [dot3(vinv[a], s[6:9]) for a in range(3)]
        p = [[quantity(g, 24 + 3 * k + c) for c in range(3)] for k in range(2)]
        e = [quantity(g, 32 + k) for k in range(2)]
        use = [[dot3(vinv[a], p[k]) for a in range(3)] for k in range(2)]
        k00 = 1.0 - dot3(p[0], use[0])
        k01 = -dot3(p[0], use[1])
        k11 = 1.0 - dot3(p[1], use[1])
        sh = [e[k] - dot3(p[k], w) for k in range(2)]
        c0 = [quantity(g, c) for c in range(9)]
        c1 = [quantity(g, 9 + c) for c in range(9)]
        for c in range(9):
            red[c, at, :] = c0[c] * sh[0] + c1[c] * sh[1]
        base = (g % 2) * (8 * TS)
        for pos, (i, j) in enumerate(PAIRS):
            if j == 0:
                a0 = k00 * c0[i] + k01 * c1[i]
                a1 = k01 * c0[i] + k11 * c1[i]
            ts[pl.ds(base + pos, 8, stride=TS), :] = a0 * c0[j] + a1 * c1[j]
        for pos in range(45, 48):
            ts[pl.ds(base + pos, 8, stride=TS), :] = jnp.zeros((8, 128), F32)

        for j in range(8):
            x = ts[base + j * TS : base + j * TS + 48, :]
            odd = jnp.broadcast_to(slot_ref[g * 8 + j : g * 8 + j + 1, :] & 1, (48, 128)) == 1
            none = jnp.zeros((16, 128), F32)
            both = [jnp.where(odd, 0.0, x), none, jnp.where(odd, x, 0.0), none]
            x = jnp.transpose(jnp.concatenate(both, axis=0))
            hi = x.astype(BF16)
            rhs[g, j * 128 : j * 128 + 128, 0:128] = hi
            rhs[g, j * 128 : j * 128 + 128, 128:256] = (x - hi.astype(F32)).astype(BF16)

    def multiply(n, g):
        for k in (2 * n, 2 * n + 1):
            count = 32 // PARTS
            lhs = one_hot(slot_ref, g, 1, k * count, count)
            part = lax.dot_general(lhs, rhs[g], (((1,), (0,)), ((), ())), preferred_element_type=F32)
            at = pl.ds(k * 16 * count, 16 * count)
            acc[at, :] = part if g == 0 else acc[at, :] + part

    terms(0)
    for g in range(8):
        multiply(0, g)
        if g < AHEAD:
            multiply(1, g)
        if g < 7:
            terms(g + 1)
    done(0)
    for g in range(AHEAD, 8):
        multiply(1, g)
    done(1)
    for g in range(8):
        multiply(2, g)
        if g == 3:
            send(0)
    done(2)
    for g in range(8):
        multiply(3, g)
        if g == 0:
            send(1)
        if g == 6:
            send(2)
    done(3)


def one_hot(slot_ref, g, shift, start, groups, mask=63, upper=None):
    iota = lax.broadcasted_iota(I32, (16, 128), 0).astype(BF16)
    zero = jnp.zeros((16, 128), BF16)
    one = jnp.ones((16, 128), BF16)
    unit, group = [], []
    for j in range(8):
        slot = jnp.broadcast_to(slot_ref[pl.ds(g * 8 + j, 1), :], (16, 128))
        low = (slot >> shift) & 15
        if upper is not None:
            low = jnp.where((slot >> 10) == upper, low, 16)
        unit.append(jnp.where(low.astype(BF16) == iota, one, zero))
        group.append(((slot >> (shift + 4)) & mask).astype(BF16))
    rows = []
    for v in range(start, start + groups):
        mine = jnp.full((16, 128), v, BF16)
        rows.append(jnp.concatenate([jnp.where(group[j] == mine, unit[j], zero) for j in range(8)], axis=1))
    return jnp.concatenate(rows, axis=0)


def invert(owned, ent, inv_ref):
    lane = lax.broadcasted_iota(I32, (128, 128), 1)
    wide = jnp.concatenate([owned] * 16, axis=0)
    spread = lane_pick(jnp.transpose(wide), (lane & 15) >> 1)
    ent[...] = jnp.where(lane[0:64] & 1 == 0, spread[0:64], spread[64:128])
    entry = {pair: ent[pl.ds(pos, 8, stride=0), :] for pos, pair in enumerate(PAIRS)}
    factor, recip = {}, {}
    for c in range(9):
        r = lax.rsqrt(entry[c, c] + 1.0 if c == 0 else entry[c, c])
        recip[c] = r
        for i in range(c + 1, 9):
            factor[i, c] = entry[i, c] * r
        for i in range(c + 1, 9):
            for j in range(c + 1, i + 1):
                base = entry[i, j] + 1.0 if (i == j and c == 0) else entry[i, j]
                entry[i, j] = base - factor[i, c] * factor[j, c]
    solved = {}
    for c in range(9):
        solved[c, c] = recip[c]
        for i in range(c + 1, 9):
            value = factor[i, c] * solved[c, c]
            for k in range(c + 1, i):
                value = value + factor[i, k] * solved[k, c]
            solved[i, c] = -value * recip[i]
    row8 = lax.broadcasted_iota(I32, (8, 128), 0)
    lane8 = lax.broadcasted_iota(I32, (8, 128), 1)
    tile = jnp.zeros((8, 128), F32)
    for pos, (i, j) in enumerate(PAIRS):
        value = solved[i, i] * solved[i, j]
        for k in range(i + 1, 9):
            value = value + solved[k, i] * solved[k, j]
        inv_ref[9 * i + j : 9 * i + j + 1, :] = value[0:1, :]
        if i != j:
            inv_ref[9 * j + i : 9 * j + i + 1, :] = value[0:1, :]
        tile = jnp.where((row8 == pos % 8) & (lane8 // 16 == pos // 8), value, tile)
    return tile


def arrange(tiles, left):
    lane = lax.broadcasted_iota(I32, (8, 128), 1)
    for h in range(8):
        x = [tiles[h * 8 + e] for e in range(8)]
        for k in (1, 2, 4):
            upper = (lane // 16) & k != 0
            for e in range(8):
                if e & k == 0:
                    low, high = x[e], x[e + k]
                    x[e] = jnp.where(upper, pltpu.roll(high, 16 * k, 1), low)
                    x[e + k] = jnp.where(upper, high, pltpu.roll(low, 128 - 16 * k, 1))
        values = jnp.concatenate(x[0:6], axis=0)
        hi = values.astype(BF16)
        lo = (values - hi.astype(F32)).astype(BF16)
        at = pl.ds(128 * (h % 2), 128)
        left[96 * (h // 2) : 96 * (h // 2) + 48, at] = hi
        left[96 * (h // 2) + 48 : 96 * (h // 2) + 96, at] = lo


def choose(left, pick_ref, g, upper, store):
    chosen = lax.dot_general(
        left[...], one_hot(pick_ref, g, 0, 0, 16, 15, upper), (((1,), (0,)), ((), ())),
        preferred_element_type=F32,
    )
    for j in range(8):
        quarter = (jnp.broadcast_to(pick_ref[g * 8 + j : g * 8 + j + 1, :], (8, 128)) >> 8) & 3
        low, high = (quarter & 1) == 1, quarter > 1
        at = slice(128 * j, 128 * j + 128)
        for r in range(0, 48, 8):
            y = [chosen[96 * q + r : 96 * q + r + 8, at] + chosen[96 * q + 48 + r : 96 * q + 56 + r, at]
                 for q in range(4)]
            store(j, r, jnp.where(high, jnp.where(low, y[3], y[2]), jnp.where(low, y[1], y[0])))


def last(theirs, pick_ref, red_ref, rows_ref, near_ref, inv_ref, out_ref, left, picked, outs):
    arrange(theirs, left)
    inv_ref[...] = jnp.transpose(rows_ref[...])[0:16, 0:81]
    for g in range(8):
        base = (g % 2) * (8 * PS)

        def store(j, r, value):
            at = (g * 8 + j) * 48 + r
            picked[base + PS * j + r : base + PS * j + r + 8, :] = value + near_ref[at : at + 8, :]

        choose(left, pick_ref, g, 1, store)
        part = [red_ref[c, g * 8 : g * 8 + 8, :] for c in range(9)]
        total = [None] * 9
        for pos, (i, j) in enumerate(PAIRS):
            value = picked[pl.ds(base + pos, 8, stride=PS), :]
            for r, c in sorted({(i, j), (j, i)}):
                x = value * part[c]
                total[r] = x if total[r] is None else total[r] + x
        base = (g % 2) * (8 * OS)
        for r in range(9):
            outs[pl.ds(base + r, 8, stride=OS), :] = total[r]
        for j in range(8):
            at = pl.ds((g * 8 + j) * 128, 128)
            out_ref[0:8, at] = outs[base + j * OS : base + j * OS + 8, :]
            out_ref[8:9, at] = outs[base + j * OS + 8 : base + j * OS + 9, :]


def kernel(cam_hbm, pt_hbm, res_hbm, pid_hbm, cid_hbm, map_hbm, rank_hbm, theirs, pick_ref, red, rows_ref, near_ref,
           cam_ref, pt_ref, res_ref, pid_ref, cid_ref, map_ref, rank_ref, pos_ref,
           xs, ts, tot, heads, tails, fix, rhs, acc, ent,
           part, swap, half, recv, owned, mine, left, load_sems, swap_sems, send_sems, recv_sems):
    pts, core = lax.axis_index("pts"), lax.axis_index("grp")
    partner = (pts, 1 - core)
    chip_z = [(((pts >> 4) + d) & 3) << 4 for d in range(4)]
    chip_x = [(((pts >> 2) + d) & 3) << 2 for d in range(4)]
    chip_y = [(pts + d) & 3 for d in range(4)]

    def chip(off):
        return chip_z[off >> 4] + chip_x[(off >> 2) & 3] + chip_y[off & 3]

    pairs = [(pt_hbm, pt_ref), (res_hbm, res_ref), (pid_hbm, pid_ref), (cid_hbm, cid_ref),
             (map_hbm, map_ref), (rank_hbm, rank_ref), (cam_hbm, cam_ref)]
    loads = [pltpu.make_async_copy(src, dst, load_sems.at[n]) for n, (src, dst) in enumerate(pairs)]
    for load in loads:
        load.start()
    barrier = pltpu.get_barrier_semaphore()
    peers = [partner] + [(chip(off), core) for off in OFFSETS[:-1]]
    peers += [(chip(off), 1 - core) for off in OFFSETS[:-1] if off in OFFSETS[CLOSE:] or back(off) in OFFSETS[CLOSE:]]
    for peer in peers:
        pl.semaphore_signal(barrier, inc=1, device_id=peer, device_id_type=MESH)

    with jax.named_scope("load"):
        for load in loads[0:3]:
            load.wait()
        spread_points(pt_ref, res_ref, xs)

    def cameras_in():
        for load in loads[3:]:
            load.wait()
        find_slots(pts, core, cid_ref, map_ref, rank_ref, pos_ref, pick_ref)
        spread_cameras(cam_ref, xs)

    def swap_of(n):
        some = pl.ds(n * EACH, EACH)
        return pltpu.make_async_remote_copy(
            src_ref=part.at[some, 1 - core], dst_ref=swap.at[some], send_sem=swap_sems.at[n],
            recv_sem=swap_sems.at[PARTS + n], device_id=partner, device_id_type=MESH)

    def give(src, slot, device):
        pltpu.make_async_remote_copy(
            src_ref=src, dst_ref=recv.at[slot], send_sem=send_sems.at[0], recv_sem=recv_sems.at[0],
            device_id=device, device_id_type=MESH).start()

    def send(n):
        swap_of(n).wait()
        for r in range(n * EACH, n * EACH + EACH):
            half[r] = part[r, core] + swap[r]
        for r in range(n * EACH, n * EACH + EACH):
            give(half.at[r], r, (chip(OFFSETS[r]), core))

    def done(n):
        with jax.named_scope("send"):
            for r in range(n * EACH, n * EACH + EACH):
                at = pl.ds(r * 16, 16)
                part[r] = (acc[at, 0:128] + acc[at, 128:256]).reshape(2, 8, 128)
            if n == 0:
                pl.semaphore_wait(barrier, len(peers))
            if n < PARTS - 1:
                swap_of(n).start()
            else:
                for r in range(CLOSE, CHIPS):
                    to = chip(OFFSETS[r])
                    if r < CHIPS - 1:
                        give(part.at[r, core], r, (to, core))
                    give(part.at[r, 1 - core], CHIPS - 1 + r - CLOSE, (to, 1 - core))

    with jax.named_scope("points"):
        point_sums(pid_ref, xs, tot, heads, tails, fix, cameras_in)
    with jax.named_scope("cameras"):
        camera_sums(pid_ref, pos_ref, xs, tot, fix, red, ts, rhs, acc, done, send)
    with jax.named_scope("scatter"):
        pltpu.make_async_copy(recv, recv, recv_sems.at[0]).wait()

    with jax.named_scope("invert"):
        sums = [recv[n] for n in range(CHIPS - 1 + EACH)] + [part[CHIPS - 1, core]]
        while len(sums) > 1:
            sums = [sums[i] + sums[i + 1] for i in range(0, len(sums) - 1, 2)] + sums[len(sums) & ~1 :]
        owned[...] = invert(sums[0], ent, rows_ref)
        mine[CHIPS - 1] = owned[...]

    with jax.named_scope("gather"):
        for off in OFFSETS[:-1]:
            pltpu.make_async_remote_copy(
                src_ref=owned, dst_ref=mine.at[RANK[back(off)]], send_sem=send_sems.at[1],
                recv_sem=recv_sems.at[1], device_id=(chip(off), core), device_id_type=MESH).start()
        others = recv.at[0 : CHIPS - 1]
        pltpu.make_async_copy(others, others, recv_sems.at[1]).wait()
    with jax.named_scope("near"):
        across = pltpu.make_async_remote_copy(
            src_ref=mine, dst_ref=theirs, send_sem=swap_sems.at[0], recv_sem=swap_sems.at[PARTS],
            device_id=partner, device_id_type=MESH)
        across.start()
        arrange(mine, left)
        for g in range(8):
            def store(j, r, value):
                at = (g * 8 + j) * 48 + r
                near_ref[at : at + 8, :] = value

            choose(left, pick_ref, g, 0, store)
    with jax.named_scope("across"):
        pltpu.make_async_copy(recv, recv, send_sems.at[0]).wait()
        pltpu.make_async_copy(others, others, send_sems.at[1]).wait()
        across.wait()


def shards(cam_jac, pt_jac, resid, obs_point, obs_camera, camera_slot):
    vm = pltpu.VMEM
    dma = pltpu.SemaphoreType.DMA
    shape = jax.ShapeDtypeStruct
    ranks = np.zeros((8, 128), np.int32)
    ranks[:, OFFSETS] = np.arange(CHIPS)
    ranks = jnp.asarray(ranks)
    theirs, picks, red, rows, near = pl.pallas_call(
        kernel,
        out_shape=(
            shape((CHIPS, 8, 128), F32),
            shape((64, 128), I32),
            shape((9, 64, 128), F32),
            shape((128, 128), F32),
            shape((64 * 48, 128), F32),
        ),
        in_specs=[pl.BlockSpec(memory_space=pltpu.HBM)] * 7,
        out_specs=[pl.BlockSpec(memory_space=vm)] * 5,
        scratch_shapes=[
            vm((18, 8192), F32),
            vm((6, 8192), F32),
            vm((2, 8192), F32),
            vm((64, 128), I32),
            vm((64, 128), I32),
            vm((16, 128), I32),
            vm((8, 128), I32),
            vm((64, 128), I32),
            vm((64 * XS, 128), F32),
            vm((16 * TS, 128), F32),
            vm((9 * 64, 128), F32),
            vm((64, 128), F32),
            vm((64, 128), F32),
            vm((128, 128), F32),
            vm((8, 1024, 256), BF16),
            vm((1024, 256), F32),
            vm((64, 128), F32),
            vm((CHIPS, 2, 8, 128), F32),
            vm((CLOSE, 8, 128), F32),
            vm((CLOSE, 8, 128), F32),
            vm((CHIPS - 1 + EACH, 8, 128), F32),
            vm((8, 128), F32),
            vm((CHIPS, 8, 128), F32),
            vm((384, 256), BF16),
            dma((7,)),
            dma((2 * PARTS,)),
            dma((2,)),
            dma((6,)),
        ],
        compiler_params=pltpu.CompilerParams(
            vmem_limit_bytes=28 * 2**20, collective_id=0, has_side_effects=True
        ),
        name="schur",
    )(
        *[
            pltpu.with_memory_space_constraint(x, pltpu.HBM)
            for x in (
                cam_jac,
                pt_jac,
                resid,
                obs_point.reshape(64, 128),
                obs_camera.reshape(64, 128),
                camera_slot.reshape(16, 128),
                ranks,
            )
        ]
    )
    inverse, precond = pl.pallas_call(
        last,
        out_shape=(shape((16, 81), F32), shape((9, 8192), F32)),
        in_specs=[pl.BlockSpec(memory_space=vm)] * 5,
        out_specs=[pl.BlockSpec(memory_space=vm)] * 2,
        scratch_shapes=[
            vm((384, 256), BF16),
            vm((16 * PS, 128), F32),
            vm((16 * OS, 128), F32),
        ],
        compiler_params=pltpu.CompilerParams(vmem_limit_bytes=28 * 2**20),
        name="last",
    )(theirs, picks, red, rows, near)
    return inverse.T, precond


def solution(mesh):
    both = ("pts", "grp")
    in_specs = (P(None, both), P(None, both), P(None, both), P(both), P(both), P())
    out_specs = (P(None, both), P(None, both))
    return jax.shard_map(shards, mesh=mesh, in_specs=in_specs, out_specs=out_specs, check_vma=False)
```

```python
import jax
import jax.numpy as jnp
import numpy as np
from jax import lax
from jax.experimental import pallas as pl
from jax.experimental.pallas import tpu as pltpu
from jax.sharding import PartitionSpec as P

F32, BF16, I32 = jnp.float32, jnp.bfloat16, jnp.int32
MESH = pl.DeviceIdType.MESH
XS = 40
TS = 56
OS = 24
PS = 56
PAIRS = [(i, j) for i in range(9) for j in range(i + 1)]
CHIPS = 64


def hops(off):
    return sum(min(d, 4 - d) for d in (off // 16, off // 4 % 4, off % 4))


OFFSETS = sorted(range(CHIPS), key=lambda off: (-hops(off), off))
RANK = {off: r for r, off in enumerate(OFFSETS)}
PARTS = 4
EACH = CHIPS // PARTS
AHEAD = 6
CLOSE = 3 * EACH


def back(off):
    return ((-(off >> 4) & 3) << 4) | ((-(off >> 2) & 3) << 2) | (-off & 3)


def m8(x):
    return pl.multiple_of(x, 8)


def lane_pick(row, idx):
    return jnp.take_along_axis(row, idx, axis=1, mode="promise_in_bounds")


def find_slots(pts, core, cid_ref, map_ref, rank_ref, pos_ref, pick_ref):
    z, x, y = pts >> 4, (pts >> 2) & 3, pts & 3
    rank = rank_ref[...]
    for g in range(8):
        cid = cid_ref[g * 8 : g * 8 + 8, :]
        lo = cid & 127
        vals = [lane_pick(map_ref[pl.ds(h, 8, stride=0), :], lo) for h in range(16)]
        for b in range(4):
            bit = ((cid >> (7 + b)) & 1) == 1
            vals = [jnp.where(bit, vals[2 * i + 1], vals[2 * i]) for i in range(len(vals) // 2)]
        slot = vals[0]
        off = ((((slot >> 9) - z) & 3) << 4) | ((((slot >> 7) - x) & 3) << 2) | (((slot >> 5) - y) & 3)
        near = lane_pick(rank, off)
        pos_ref[g * 8 : g * 8 + 8, :] = (near << 5) | (slot & 31)
        pick_ref[g * 8 : g * 8 + 8, :] = ((((slot >> 4) & 1) ^ core) << 10) | (near << 4) | (slot & 15)


def spread_points(pt_ref, res_ref, xs):
    for j in range(64):
        at = pl.ds(j * 128, 128)
        xs[j * XS + 24 : j * XS + 30, :] = pt_ref[0:6, at]
        xs[j * XS + 32 : j * XS + 34, :] = res_ref[0:2, at]


def spread_cameras(cam_ref, xs):
    for j in range(64):
        at = pl.ds(j * 128, 128)
        xs[j * XS : j * XS + 8, :] = cam_ref[0:8, at]
        xs[j * XS + 8 : j * XS + 16, :] = cam_ref[8:16, at]
        xs[j * XS + 16 : j * XS + 18, :] = cam_ref[16:18, at]


def point_sums(pid_ref, xs, tot, heads, tails, fix, between):
    lane = lax.broadcasted_iota(I32, (8, 128), 1)

    def quantity(g, q):
        return xs[pl.ds(g * (8 * XS) + q, 8, stride=XS), :]

    def one(g):
        p = [[quantity(g, 24 + 3 * k + c) for c in range(3)] for k in range(2)]
        e = [quantity(g, 32 + k) for k in range(2)]
        pid = pid_ref[pl.ds(m8(g * 8), 8), :]
        v = [p[0][a] * p[0][c] + p[1][a] * p[1][c] for a in range(3) for c in range(a, 3)]
        v += [p[0][a] * e[0] + p[1][a] * e[1] for a in range(3)]
        return pid, v, lane

    def scan(state, k):
        pid, v, end = state
        same = (pltpu.roll(pid, k, 1) == pid) & (lane >= k)
        v = [x + jnp.where(same, pltpu.roll(x, k, 1), 0.0) for x in v]
        after = (pltpu.roll(pid, 128 - k, 1) == pid) & (lane < 128 - k)
        return pid, v, jnp.where(after, pltpu.roll(end, 128 - k, 1), end)

    def finish(g, state):
        pid, v, end = state
        head = jnp.zeros((8, 128), F32)
        tail = jnp.zeros((8, 128), F32)
        for q in range(9):
            full = lane_pick(v[q], end)
            tot[pl.ds(m8(q * 64 + g * 8), 8), :] = full
            ends = pltpu.roll(full, q + 1, 1)
            head = jnp.where(lane == q + 1, ends, head)
            tail = jnp.where(lane == q, ends, tail)
        heads[pl.ds(m8(g * 8), 8), :] = head
        tails[pl.ds(m8(g * 8), 8), :] = tail

    states = [one(g) for g in range(8)]
    for b in range(7):
        states = [scan(state, 1 << b) for state in states]
    for g in range(8):
        finish(g, states[g])
    between()

    pid = pid_ref[...]
    first = jnp.broadcast_to(pid[:, 0:1], (64, 128))
    last = jnp.broadcast_to(pid[:, 127:128], (64, 128))
    ends = jnp.where(lax.broadcasted_iota(I32, (64, 128), 1) < 64, first, last).astype(F32)
    across = jnp.transpose(ends)
    r0 = lax.broadcasted_iota(I32, (64, 64), 0)
    r1 = lax.broadcasted_iota(I32, (64, 64), 1)
    from_before = (r1 < r0) & (across[64:128, :] == first[:, 0:64].astype(F32))
    from_after = (r1 > r0) & (across[0:64, :] == last[:, 0:64].astype(F32))

    def total(which, values):
        return lax.dot_general(
            jnp.where(which, 1.0, 0.0),
            values[...],
            (((1,), (0,)), ((), ())),
            precision=lax.Precision.HIGHEST,
            preferred_element_type=F32,
        )

    fix[0:64, :] = total(from_before, tails)
    fix[64:128, :] = total(from_after, heads)


def camera_sums(pid_ref, slot_ref, xs, tot, fix, red, ts, rhs, acc, done, send):
    def quantity(g, q):
        return xs[pl.ds(g * (8 * XS) + q, 8, stride=XS), :]

    def dot3(a, b):
        return a[0] * b[0] + a[1] * b[1] + a[2] * b[2]

    def terms(g):
        at = pl.ds(g * 8, 8)
        pid = pid_ref[at, :]
        pre = fix[at, :]
        post = fix[pl.ds(64 + g * 8, 8), :]
        is_first = pid == jnp.broadcast_to(pid[:, 0:1], (8, 128))
        is_last = pid == jnp.broadcast_to(pid[:, 127:128], (8, 128))
        s = []
        for q in range(9):
            x = tot[pl.ds(q * 64 + g * 8, 8), :]
            x = x + jnp.where(is_first, jnp.broadcast_to(pre[:, q : q + 1], (8, 128)), 0.0)
            x = x + jnp.where(is_last, jnp.broadcast_to(post[:, q + 1 : q + 2], (8, 128)), 0.0)
            s.append(x)
        v00, v01, v02, v11, v12, v22 = s[0] + 1.0, s[1], s[2], s[3] + 1.0, s[4], s[5] + 1.0
        c00 = v11 * v22 - v12 * v12
        c01 = v02 * v12 - v01 * v22
        c02 = v01 * v12 - v02 * v11
        c11 = v00 * v22 - v02 * v02
        c12 = v01 * v02 - v00 * v12
        c22 = v00 * v11 - v01 * v01
        inv = 1.0 / (v00 * c00 + v01 * c01 + v02 * c02)
        i00, i01, i02, i11, i12, i22 = [c * inv for c in (c00, c01, c02, c11, c12, c22)]
        vinv = ((i00, i01, i02), (i01, i11, i12), (i02, i12, i22))
        w = [dot3(vinv[a], s[6:9]) for a in range(3)]
        p = [[quantity(g, 24 + 3 * k + c) for c in range(3)] for k in range(2)]
        e = [quantity(g, 32 + k) for k in range(2)]
        use = [[dot3(vinv[a], p[k]) for a in range(3)] for k in range(2)]
        k00 = 1.0 - dot3(p[0], use[0])
        k01 = -dot3(p[0], use[1])
        k11 = 1.0 - dot3(p[1], use[1])
        sh = [e[k] - dot3(p[k], w) for k in range(2)]
        c0 = [quantity(g, c) for c in range(9)]
        c1 = [quantity(g, 9 + c) for c in range(9)]
        for c in range(9):
            red[c, at, :] = c0[c] * sh[0] + c1[c] * sh[1]
        base = (g % 2) * (8 * TS)
        for pos, (i, j) in enumerate(PAIRS):
            if j == 0:
                a0 = k00 * c0[i] + k01 * c1[i]
                a1 = k01 * c0[i] + k11 * c1[i]
            ts[pl.ds(base + pos, 8, stride=TS), :] = a0 * c0[j] + a1 * c1[j]
        for pos in range(45, 48):
            ts[pl.ds(base + pos, 8, stride=TS), :] = jnp.zeros((8, 128), F32)

        for j in range(8):
            x = ts[base + j * TS : base + j * TS + 48, :]
            odd = jnp.broadcast_to(slot_ref[g * 8 + j : g * 8 + j + 1, :] & 1, (48, 128)) == 1
            none = jnp.zeros((16, 128), F32)
            both = [jnp.where(odd, 0.0, x), none, jnp.where(odd, x, 0.0), none]
            x = jnp.transpose(jnp.concatenate(both, axis=0))
            hi = x.astype(BF16)
            rhs[g, j * 128 : j * 128 + 128, 0:128] = hi
            rhs[g, j * 128 : j * 128 + 128, 128:256] = (x - hi.astype(F32)).astype(BF16)

    def multiply(n, g):
        for k in (2 * n, 2 * n + 1):
            count = 32 // PARTS
            lhs = one_hot(slot_ref, g, 1, k * count, count)
            part = lax.dot_general(lhs, rhs[g], (((1,), (0,)), ((), ())), preferred_element_type=F32)
            at = pl.ds(k * 16 * count, 16 * count)
            acc[at, :] = part if g == 0 else acc[at, :] + part

    terms(0)
    terms(1)
    for g in range(8):
        multiply(0, g)
        if g < AHEAD:
            multiply(1, g)
        if g < 6:
            terms(g + 2)
    done(0)
    for g in range(AHEAD, 8):
        multiply(1, g)
    done(1)
    for g in range(8):
        multiply(2, g)
        if g == 3:
            send(0)
    done(2)
    for g in range(8):
        multiply(3, g)
        if g == 0:
            send(1)
        if g == 6:
            send(2)
    done(3)


def one_hot(slot_ref, g, shift, start, groups, mask=63, upper=None):
    iota = lax.broadcasted_iota(I32, (16, 128), 0).astype(BF16)
    zero = jnp.zeros((16, 128), BF16)
    one = jnp.ones((16, 128), BF16)
    unit, group = [], []
    for j in range(8):
        slot = jnp.broadcast_to(slot_ref[pl.ds(g * 8 + j, 1), :], (16, 128))
        low = (slot >> shift) & 15
        if upper is not None:
            low = jnp.where((slot >> 10) == upper, low, 16)
        unit.append(jnp.where(low.astype(BF16) == iota, one, zero))
        group.append(((slot >> (shift + 4)) & mask).astype(BF16))
    rows = []
    for v in range(start, start + groups):
        mine = jnp.full((16, 128), v, BF16)
        rows.append(jnp.concatenate([jnp.where(group[j] == mine, unit[j], zero) for j in range(8)], axis=1))
    return jnp.concatenate(rows, axis=0)


def invert(owned, ent, inv_ref):
    lane = lax.broadcasted_iota(I32, (128, 128), 1)
    wide = jnp.concatenate([owned] * 16, axis=0)
    spread = lane_pick(jnp.transpose(wide), (lane & 15) >> 1)
    ent[...] = jnp.where(lane[0:64] & 1 == 0, spread[0:64], spread[64:128])
    entry = {pair: ent[pl.ds(pos, 8, stride=0), :] for pos, pair in enumerate(PAIRS)}
    factor, recip = {}, {}
    for c in range(9):
        r = lax.rsqrt(entry[c, c] + 1.0 if c == 0 else entry[c, c])
        recip[c] = r
        for i in range(c + 1, 9):
            factor[i, c] = entry[i, c] * r
        for i in range(c + 1, 9):
            for j in range(c + 1, i + 1):
                base = entry[i, j] + 1.0 if (i == j and c == 0) else entry[i, j]
                entry[i, j] = base - factor[i, c] * factor[j, c]
    solved = {}
    for c in range(9):
        solved[c, c] = recip[c]
        for i in range(c + 1, 9):
            value = factor[i, c] * solved[c, c]
            for k in range(c + 1, i):
                value = value + factor[i, k] * solved[k, c]
            solved[i, c] = -value * recip[i]
    row8 = lax.broadcasted_iota(I32, (8, 128), 0)
    lane8 = lax.broadcasted_iota(I32, (8, 128), 1)
    tile = jnp.zeros((8, 128), F32)
    for pos, (i, j) in enumerate(PAIRS):
        value = solved[i, i] * solved[i, j]
        for k in range(i + 1, 9):
            value = value + solved[k, i] * solved[k, j]
        inv_ref[9 * i + j : 9 * i + j + 1, :] = value[0:1, :]
        if i != j:
            inv_ref[9 * j + i : 9 * j + i + 1, :] = value[0:1, :]
        tile = jnp.where((row8 == pos % 8) & (lane8 // 16 == pos // 8), value, tile)
    return tile


def arrange(tiles, left):
    lane = lax.broadcasted_iota(I32, (8, 128), 1)
    for h in range(8):
        x = [tiles[h * 8 + e] for e in range(8)]
        for k in (1, 2, 4):
            upper = (lane // 16) & k != 0
            for e in range(8):
                if e & k == 0:
                    low, high = x[e], x[e + k]
                    x[e] = jnp.where(upper, pltpu.roll(high, 16 * k, 1), low)
                    x[e + k] = jnp.where(upper, high, pltpu.roll(low, 128 - 16 * k, 1))
        values = jnp.concatenate(x[0:6], axis=0)
        hi = values.astype(BF16)
        lo = (values - hi.astype(F32)).astype(BF16)
        at = pl.ds(128 * (h % 2), 128)
        left[96 * (h // 2) : 96 * (h // 2) + 48, at] = hi
        left[96 * (h // 2) + 48 : 96 * (h // 2) + 96, at] = lo


def choose(left, pick_ref, g, upper, store):
    chosen = lax.dot_general(
        left[...], one_hot(pick_ref, g, 0, 0, 16, 15, upper), (((1,), (0,)), ((), ())),
        preferred_element_type=F32,
    )
    for j in range(8):
        quarter = (jnp.broadcast_to(pick_ref[g * 8 + j : g * 8 + j + 1, :], (8, 128)) >> 8) & 3
        low, high = (quarter & 1) == 1, quarter > 1
        at = slice(128 * j, 128 * j + 128)
        for r in range(0, 48, 8):
            y = [chosen[96 * q + r : 96 * q + r + 8, at] + chosen[96 * q + 48 + r : 96 * q + 56 + r, at]
                 for q in range(4)]
            store(j, r, jnp.where(high, jnp.where(low, y[3], y[2]), jnp.where(low, y[1], y[0])))


def last(theirs, pick_ref, red_ref, rows_ref, near_ref, inv_ref, out_ref, left, picked, outs):
    arrange(theirs, left)
    inv_ref[...] = jnp.transpose(rows_ref[...])[0:16, 0:81]
    for g in range(8):
        base = (g % 2) * (8 * PS)

        def store(j, r, value):
            at = (g * 8 + j) * 48 + r
            picked[base + PS * j + r : base + PS * j + r + 8, :] = value + near_ref[at : at + 8, :]

        choose(left, pick_ref, g, 1, store)
        part = [red_ref[c, g * 8 : g * 8 + 8, :] for c in range(9)]
        total = [None] * 9
        for pos, (i, j) in enumerate(PAIRS):
            value = picked[pl.ds(base + pos, 8, stride=PS), :]
            for r, c in sorted({(i, j), (j, i)}):
                x = value * part[c]
                total[r] = x if total[r] is None else total[r] + x
        base = (g % 2) * (8 * OS)
        for r in range(9):
            outs[pl.ds(base + r, 8, stride=OS), :] = total[r]
        for j in range(8):
            at = pl.ds((g * 8 + j) * 128, 128)
            out_ref[0:8, at] = outs[base + j * OS : base + j * OS + 8, :]
            out_ref[8:9, at] = outs[base + j * OS + 8 : base + j * OS + 9, :]


def kernel(cam_hbm, pt_hbm, res_hbm, pid_hbm, cid_hbm, map_hbm, rank_hbm, theirs, pick_ref, red, rows_ref, near_ref,
           cam_ref, pt_ref, res_ref, pid_ref, cid_ref, map_ref, rank_ref, pos_ref,
           xs, ts, tot, heads, tails, fix, rhs, acc, ent,
           part, swap, half, recv, owned, mine, left, load_sems, swap_sems, send_sems, recv_sems):
    pts, core = lax.axis_index("pts"), lax.axis_index("grp")
    partner = (pts, 1 - core)
    chip_z = [(((pts >> 4) + d) & 3) << 4 for d in range(4)]
    chip_x = [(((pts >> 2) + d) & 3) << 2 for d in range(4)]
    chip_y = [(pts + d) & 3 for d in range(4)]

    def chip(off):
        return chip_z[off >> 4] + chip_x[(off >> 2) & 3] + chip_y[off & 3]

    pairs = [(pt_hbm, pt_ref), (res_hbm, res_ref), (pid_hbm, pid_ref), (cid_hbm, cid_ref),
             (map_hbm, map_ref), (rank_hbm, rank_ref), (cam_hbm, cam_ref)]
    loads = [pltpu.make_async_copy(src, dst, load_sems.at[n]) for n, (src, dst) in enumerate(pairs)]
    for load in loads[0:6]:
        load.start()
    barrier = pltpu.get_barrier_semaphore()
    peers = [partner] + [(chip(off), core) for off in OFFSETS[:-1]]
    peers += [(chip(off), 1 - core) for off in OFFSETS[:-1] if off in OFFSETS[CLOSE:] or back(off) in OFFSETS[CLOSE:]]
    for peer in peers:
        pl.semaphore_signal(barrier, inc=1, device_id=peer, device_id_type=MESH)
    loads[6].start()

    with jax.named_scope("load"):
        for load in loads[0:3]:
            load.wait()
        spread_points(pt_ref, res_ref, xs)

    def cameras_in():
        for load in loads[3:]:
            load.wait()
        find_slots(pts, core, cid_ref, map_ref, rank_ref, pos_ref, pick_ref)
        spread_cameras(cam_ref, xs)

    def swap_of(n):
        some = pl.ds(n * EACH, EACH)
        return pltpu.make_async_remote_copy(
            src_ref=part.at[some, 1 - core], dst_ref=swap.at[some], send_sem=swap_sems.at[n],
            recv_sem=swap_sems.at[PARTS + n], device_id=partner, device_id_type=MESH)

    def give(src, slot, device):
        pltpu.make_async_remote_copy(
            src_ref=src, dst_ref=recv.at[slot], send_sem=send_sems.at[0], recv_sem=recv_sems.at[0],
            device_id=device, device_id_type=MESH).start()

    def send(n):
        swap_of(n).wait()
        for r in range(n * EACH, n * EACH + EACH):
            half[r] = part[r, core] + swap[r]
        for r in range(n * EACH, n * EACH + EACH):
            give(half.at[r], r, (chip(OFFSETS[r]), core))

    def done(n):
        with jax.named_scope("send"):
            for r in range(n * EACH, n * EACH + EACH):
                at = pl.ds(r * 16, 16)
                part[r] = (acc[at, 0:128] + acc[at, 128:256]).reshape(2, 8, 128)
            if n == 0:
                pl.semaphore_wait(barrier, len(peers))
            if n < PARTS - 1:
                swap_of(n).start()
            else:
                for r in range(CLOSE, CHIPS):
                    to = chip(OFFSETS[r])
                    if r < CHIPS - 1:
                        give(part.at[r, core], r, (to, core))
                    give(part.at[r, 1 - core], CHIPS - 1 + r - CLOSE, (to, 1 - core))

    with jax.named_scope("points"):
        point_sums(pid_ref, xs, tot, heads, tails, fix, cameras_in)
    with jax.named_scope("cameras"):
        camera_sums(pid_ref, pos_ref, xs, tot, fix, red, ts, rhs, acc, done, send)
    with jax.named_scope("scatter"):
        pltpu.make_async_copy(recv, recv, recv_sems.at[0]).wait()

    with jax.named_scope("invert"):
        sums = [recv[n] for n in range(CHIPS - 1 + EACH)] + [part[CHIPS - 1, core]]
        while len(sums) > 1:
            sums = [sums[i] + sums[i + 1] for i in range(0, len(sums) - 1, 2)] + sums[len(sums) & ~1 :]
        owned[...] = invert(sums[0], ent, rows_ref)
        mine[CHIPS - 1] = owned[...]

    with jax.named_scope("gather"):
        for off in OFFSETS[:-1]:
            pltpu.make_async_remote_copy(
                src_ref=owned, dst_ref=mine.at[RANK[back(off)]], send_sem=send_sems.at[1],
                recv_sem=recv_sems.at[1], device_id=(chip(off), core), device_id_type=MESH).start()
        others = recv.at[0 : CHIPS - 1]
        pltpu.make_async_copy(others, others, recv_sems.at[1]).wait()
    with jax.named_scope("near"):
        across = pltpu.make_async_remote_copy(
            src_ref=mine, dst_ref=theirs, send_sem=swap_sems.at[0], recv_sem=swap_sems.at[PARTS],
            device_id=partner, device_id_type=MESH)
        across.start()
        arrange(mine, left)
        for g in range(8):
            def store(j, r, value):
                at = (g * 8 + j) * 48 + r
                near_ref[at : at + 8, :] = value

            choose(left, pick_ref, g, 0, store)
    with jax.named_scope("across"):
        pltpu.make_async_copy(recv, recv, send_sems.at[0]).wait()
        pltpu.make_async_copy(others, others, send_sems.at[1]).wait()
        across.wait()


def shards(cam_jac, pt_jac, resid, obs_point, obs_camera, camera_slot):
    vm = pltpu.VMEM
    dma = pltpu.SemaphoreType.DMA
    shape = jax.ShapeDtypeStruct
    ranks = np.zeros((8, 128), np.int32)
    ranks[:, OFFSETS] = np.arange(CHIPS)
    ranks = jnp.asarray(ranks)
    theirs, picks, red, rows, near = pl.pallas_call(
        kernel,
        out_shape=(
            shape((CHIPS, 8, 128), F32),
            shape((64, 128), I32),
            shape((9, 64, 128), F32),
            shape((128, 128), F32),
            shape((64 * 48, 128), F32),
        ),
        in_specs=[pl.BlockSpec(memory_space=pltpu.HBM)] * 7,
        out_specs=[pl.BlockSpec(memory_space=vm)] * 5,
        scratch_shapes=[
            vm((18, 8192), F32),
            vm((6, 8192), F32),
            vm((2, 8192), F32),
            vm((64, 128), I32),
            vm((64, 128), I32),
            vm((16, 128), I32),
            vm((8, 128), I32),
            vm((64, 128), I32),
            vm((64 * XS, 128), F32),
            vm((16 * TS, 128), F32),
            vm((9 * 64, 128), F32),
            vm((64, 128), F32),
            vm((64, 128), F32),
            vm((128, 128), F32),
            vm((8, 1024, 256), BF16),
            vm((1024, 256), F32),
            vm((64, 128), F32),
            vm((CHIPS, 2, 8, 128), F32),
            vm((CLOSE, 8, 128), F32),
            vm((CLOSE, 8, 128), F32),
            vm((CHIPS - 1 + EACH, 8, 128), F32),
            vm((8, 128), F32),
            vm((CHIPS, 8, 128), F32),
            vm((384, 256), BF16),
            dma((7,)),
            dma((2 * PARTS,)),
            dma((2,)),
            dma((6,)),
        ],
        compiler_params=pltpu.CompilerParams(
            vmem_limit_bytes=28 * 2**20, collective_id=0, has_side_effects=True
        ),
        name="schur",
    )(
        *[
            pltpu.with_memory_space_constraint(x, pltpu.HBM)
            for x in (
                cam_jac,
                pt_jac,
                resid,
                obs_point.reshape(64, 128),
                obs_camera.reshape(64, 128),
                camera_slot.reshape(16, 128),
                ranks,
            )
        ]
    )
    inverse, precond = pl.pallas_call(
        last,
        out_shape=(shape((16, 81), F32), shape((9, 8192), F32)),
        in_specs=[pl.BlockSpec(memory_space=vm)] * 5,
        out_specs=[pl.BlockSpec(memory_space=vm)] * 2,
        scratch_shapes=[
            vm((384, 256), BF16),
            vm((16 * PS, 128), F32),
            vm((16 * OS, 128), F32),
        ],
        compiler_params=pltpu.CompilerParams(vmem_limit_bytes=28 * 2**20),
        name="last",
    )(theirs, picks, red, rows, near)
    return inverse.T, precond


def solution(mesh):
    both = ("pts", "grp")
    in_specs = (P(None, both), P(None, both), P(None, both), P(both), P(both), P())
    out_specs = (P(None, both), P(None, both))
    return jax.shard_map(shards, mesh=mesh, in_specs=in_specs, out_specs=out_specs, check_vma=False)
```

```python
import jax
import jax.numpy as jnp
import numpy as np
from jax import lax
from jax.experimental import pallas as pl
from jax.experimental.pallas import tpu as pltpu
from jax.sharding import PartitionSpec as P

F32, BF16, I32 = jnp.float32, jnp.bfloat16, jnp.int32
MESH = pl.DeviceIdType.MESH
XS = 40
TS = 56
OS = 24
PS = 56
PAIRS = [(i, j) for i in range(9) for j in range(i + 1)]
CHIPS = 64


def hops(off):
    return sum(min(d, 4 - d) for d in (off // 16, off // 4 % 4, off % 4))


OFFSETS = sorted(range(CHIPS), key=lambda off: (-hops(off), off))
RANK = {off: r for r, off in enumerate(OFFSETS)}
PARTS = 4
EACH = CHIPS // PARTS
AHEAD = 6
CLOSE = 3 * EACH


def back(off):
    return ((-(off >> 4) & 3) << 4) | ((-(off >> 2) & 3) << 2) | (-off & 3)


def m8(x):
    return pl.multiple_of(x, 8)


def lane_pick(row, idx):
    return jnp.take_along_axis(row, idx, axis=1, mode="promise_in_bounds")


def find_slots(pts, core, cid_ref, map_ref, rank_ref, pos_ref, pick_ref):
    z, x, y = pts >> 4, (pts >> 2) & 3, pts & 3
    rank = rank_ref[...]
    for g in range(8):
        cid = cid_ref[g * 8 : g * 8 + 8, :]
        lo = cid & 127
        vals = [lane_pick(map_ref[pl.ds(h, 8, stride=0), :], lo) for h in range(16)]
        for b in range(4):
            bit = ((cid >> (7 + b)) & 1) == 1
            vals = [jnp.where(bit, vals[2 * i + 1], vals[2 * i]) for i in range(len(vals) // 2)]
        slot = vals[0]
        off = ((((slot >> 9) - z) & 3) << 4) | ((((slot >> 7) - x) & 3) << 2) | (((slot >> 5) - y) & 3)
        near = lane_pick(rank, off)
        pos_ref[g * 8 : g * 8 + 8, :] = (near << 5) | (slot & 31)
        pick_ref[g * 8 : g * 8 + 8, :] = ((((slot >> 4) & 1) ^ core) << 10) | (near << 4) | (slot & 15)


def spread_points(pt_ref, res_ref, xs):
    for j in range(64):
        at = pl.ds(j * 128, 128)
        xs[j * XS + 24 : j * XS + 30, :] = pt_ref[0:6, at]
        xs[j * XS + 32 : j * XS + 34, :] = res_ref[0:2, at]


def spread_cameras(cam_ref, xs):
    for j in range(64):
        at = pl.ds(j * 128, 128)
        xs[j * XS : j * XS + 8, :] = cam_ref[0:8, at]
        xs[j * XS + 8 : j * XS + 16, :] = cam_ref[8:16, at]
        xs[j * XS + 16 : j * XS + 18, :] = cam_ref[16:18, at]


def point_sums(pid_ref, xs, tot, heads, tails, fix, between):
    lane = lax.broadcasted_iota(I32, (8, 128), 1)

    def quantity(g, q):
        return xs[pl.ds(g * (8 * XS) + q, 8, stride=XS), :]

    def one(g):
        p = [[quantity(g, 24 + 3 * k + c) for c in range(3)] for k in range(2)]
        e = [quantity(g, 32 + k) for k in range(2)]
        pid = pid_ref[pl.ds(m8(g * 8), 8), :]
        v = [p[0][a] * p[0][c] + p[1][a] * p[1][c] for a in range(3) for c in range(a, 3)]
        v += [p[0][a] * e[0] + p[1][a] * e[1] for a in range(3)]
        return pid, v, lane

    def scan(state, k):
        pid, v, end = state
        same = (pltpu.roll(pid, k, 1) == pid) & (lane >= k)
        v = [x + jnp.where(same, pltpu.roll(x, k, 1), 0.0) for x in v]
        after = (pltpu.roll(pid, 128 - k, 1) == pid) & (lane < 128 - k)
        return pid, v, jnp.where(after, pltpu.roll(end, 128 - k, 1), end)

    def finish(g, state):
        pid, v, end = state
        head = jnp.zeros((8, 128), F32)
        tail = jnp.zeros((8, 128), F32)
        for q in range(9):
            full = lane_pick(v[q], end)
            tot[pl.ds(m8(q * 64 + g * 8), 8), :] = full
            ends = pltpu.roll(full, q + 1, 1)
            head = jnp.where(lane == q + 1, ends, head)
            tail = jnp.where(lane == q, ends, tail)
        heads[pl.ds(m8(g * 8), 8), :] = head
        tails[pl.ds(m8(g * 8), 8), :] = tail

    states = [one(g) for g in range(8)]
    for b in range(7):
        states = [scan(state, 1 << b) for state in states]
    for g in range(8):
        finish(g, states[g])
    between()

    pid = pid_ref[...]
    first = jnp.broadcast_to(pid[:, 0:1], (64, 128))
    last = jnp.broadcast_to(pid[:, 127:128], (64, 128))
    ends = jnp.where(lax.broadcasted_iota(I32, (64, 128), 1) < 64, first, last).astype(F32)
    across = jnp.transpose(ends)
    r0 = lax.broadcasted_iota(I32, (64, 64), 0)
    r1 = lax.broadcasted_iota(I32, (64, 64), 1)
    from_before = (r1 < r0) & (across[64:128, :] == first[:, 0:64].astype(F32))
    from_after = (r1 > r0) & (across[0:64, :] == last[:, 0:64].astype(F32))

    def total(which, values):
        return lax.dot_general(
            jnp.where(which, 1.0, 0.0),
            values[...],
            (((1,), (0,)), ((), ())),
            precision=lax.Precision.HIGHEST,
            preferred_element_type=F32,
        )

    fix[0:64, :] = total(from_before, tails)
    fix[64:128, :] = total(from_after, heads)


def camera_sums(pid_ref, slot_ref, xs, tot, fix, red, ts, rhs, acc, done, send):
    def quantity(g, q):
        return xs[pl.ds(g * (8 * XS) + q, 8, stride=XS), :]

    def dot3(a, b):
        return a[0] * b[0] + a[1] * b[1] + a[2] * b[2]

    def terms(g):
        at = pl.ds(g * 8, 8)
        pid = pid_ref[at, :]
        pre = fix[at, :]
        post = fix[pl.ds(64 + g * 8, 8), :]
        is_first = pid == jnp.broadcast_to(pid[:, 0:1], (8, 128))
        is_last = pid == jnp.broadcast_to(pid[:, 127:128], (8, 128))
        s = []
        for q in range(9):
            x = tot[pl.ds(q * 64 + g * 8, 8), :]
            x = x + jnp.where(is_first, jnp.broadcast_to(pre[:, q : q + 1], (8, 128)), 0.0)
            x = x + jnp.where(is_last, jnp.broadcast_to(post[:, q + 1 : q + 2], (8, 128)), 0.0)
            s.append(x)
        v00, v01, v02, v11, v12, v22 = s[0] + 1.0, s[1], s[2], s[3] + 1.0, s[4], s[5] + 1.0
        c00 = v11 * v22 - v12 * v12
        c01 = v02 * v12 - v01 * v22
        c02 = v01 * v12 - v02 * v11
        c11 = v00 * v22 - v02 * v02
        c12 = v01 * v02 - v00 * v12
        c22 = v00 * v11 - v01 * v01
        inv = 1.0 / (v00 * c00 + v01 * c01 + v02 * c02)
        i00, i01, i02, i11, i12, i22 = [c * inv for c in (c00, c01, c02, c11, c12, c22)]
        vinv = ((i00, i01, i02), (i01, i11, i12), (i02, i12, i22))
        w = [dot3(vinv[a], s[6:9]) for a in range(3)]
        p = [[quantity(g, 24 + 3 * k + c) for c in range(3)] for k in range(2)]
        e = [quantity(g, 32 + k) for k in range(2)]
        use = [[dot3(vinv[a], p[k]) for a in range(3)] for k in range(2)]
        k00 = 1.0 - dot3(p[0], use[0])
        k01 = -dot3(p[0], use[1])
        k11 = 1.0 - dot3(p[1], use[1])
        sh = [e[k] - dot3(p[k], w) for k in range(2)]
        c0 = [quantity(g, c) for c in range(9)]
        c1 = [quantity(g, 9 + c) for c in range(9)]
        for c in range(9):
            red[c, at, :] = c0[c] * sh[0] + c1[c] * sh[1]
        base = (g % 2) * (8 * TS)
        for pos, (i, j) in enumerate(PAIRS):
            if j == 0:
                a0 = k00 * c0[i] + k01 * c1[i]
                a1 = k01 * c0[i] + k11 * c1[i]
            ts[pl.ds(base + pos, 8, stride=TS), :] = a0 * c0[j] + a1 * c1[j]
        for pos in range(45, 48):
            ts[pl.ds(base + pos, 8, stride=TS), :] = jnp.zeros((8, 128), F32)

        for j in range(8):
            x = ts[base + j * TS : base + j * TS + 48, :]
            odd = jnp.broadcast_to(slot_ref[g * 8 + j : g * 8 + j + 1, :] & 1, (48, 128)) == 1
            none = jnp.zeros((16, 128), F32)
            both = [jnp.where(odd, 0.0, x), none, jnp.where(odd, x, 0.0), none]
            x = jnp.transpose(jnp.concatenate(both, axis=0))
            hi = x.astype(BF16)
            rhs[g, j * 128 : j * 128 + 128, 0:128] = hi
            rhs[g, j * 128 : j * 128 + 128, 128:256] = (x - hi.astype(F32)).astype(BF16)

    def multiply(n, g):
        for k in (2 * n, 2 * n + 1):
            count = 32 // PARTS
            lhs = one_hot(slot_ref, g, 1, k * count, count)
            part = lax.dot_general(lhs, rhs[g], (((1,), (0,)), ((), ())), preferred_element_type=F32)
            at = pl.ds(k * 16 * count, 16 * count)
            acc[at, :] = part if g == 0 else acc[at, :] + part

    terms(0)
    terms(1)
    for g in range(8):
        multiply(0, g)
        if g < AHEAD:
            multiply(1, g)
        if g < 6:
            terms(g + 2)
    done(0)
    for g in range(AHEAD, 8):
        multiply(1, g)
    done(1)
    for g in range(8):
        multiply(2, g)
        if g == 3:
            send(0)
    done(2)
    for g in range(8):
        multiply(3, g)
        if g == 0:
            send(1)
        if g == 6:
            send(2)
    done(3)


def one_hot(slot_ref, g, shift, start, groups, mask=63, upper=None):
    iota = lax.broadcasted_iota(I32, (16, 128), 0).astype(BF16)
    zero = jnp.zeros((16, 128), BF16)
    one = jnp.ones((16, 128), BF16)
    unit, group = [], []
    for j in range(8):
        slot = jnp.broadcast_to(slot_ref[pl.ds(g * 8 + j, 1), :], (16, 128))
        low = (slot >> shift) & 15
        if upper is not None:
            low = jnp.where((slot >> 10) == upper, low, 16)
        unit.append(jnp.where(low.astype(BF16) == iota, one, zero))
        group.append(((slot >> (shift + 4)) & mask).astype(BF16))
    rows = []
    for v in range(start, start + groups):
        mine = jnp.full((16, 128), v, BF16)
        rows.append(jnp.concatenate([jnp.where(group[j] == mine, unit[j], zero) for j in range(8)], axis=1))
    return jnp.concatenate(rows, axis=0)


def invert(owned, ent, inv_ref):
    lane = lax.broadcasted_iota(I32, (128, 128), 1)
    wide = jnp.concatenate([owned] * 16, axis=0)
    spread = lane_pick(jnp.transpose(wide), (lane & 15) >> 1)
    ent[...] = jnp.where(lane[0:64] & 1 == 0, spread[0:64], spread[64:128])
    entry = {pair: ent[pl.ds(pos, 8, stride=0), :] for pos, pair in enumerate(PAIRS)}
    factor, recip = {}, {}
    for c in range(9):
        r = lax.rsqrt(entry[c, c] + 1.0 if c == 0 else entry[c, c])
        recip[c] = r
        for i in range(c + 1, 9):
            factor[i, c] = entry[i, c] * r
        for i in range(c + 1, 9):
            for j in range(c + 1, i + 1):
                base = entry[i, j] + 1.0 if (i == j and c == 0) else entry[i, j]
                entry[i, j] = base - factor[i, c] * factor[j, c]
    solved = {}
    for c in range(9):
        solved[c, c] = recip[c]
        for i in range(c + 1, 9):
            value = factor[i, c] * solved[c, c]
            for k in range(c + 1, i):
                value = value + factor[i, k] * solved[k, c]
            solved[i, c] = -value * recip[i]
    row8 = lax.broadcasted_iota(I32, (8, 128), 0)
    lane8 = lax.broadcasted_iota(I32, (8, 128), 1)
    tile = jnp.zeros((8, 128), F32)
    for pos, (i, j) in enumerate(PAIRS):
        value = solved[i, i] * solved[i, j]
        for k in range(i + 1, 9):
            value = value + solved[k, i] * solved[k, j]
        inv_ref[9 * i + j : 9 * i + j + 1, :] = value[0:1, :]
        if i != j:
            inv_ref[9 * j + i : 9 * j + i + 1, :] = value[0:1, :]
        tile = jnp.where((row8 == pos % 8) & (lane8 // 16 == pos // 8), value, tile)
    return tile


def arrange(tiles, table):
    lane = lax.broadcasted_iota(I32, (8, 128), 1)
    for h in range(8):
        x = [tiles[h * 8 + e] for e in range(8)]
        for k in (1, 2, 4):
            upper = (lane // 16) & k != 0
            for e in range(8):
                if e & k == 0:
                    low, high = x[e], x[e + k]
                    x[e] = jnp.where(upper, pltpu.roll(high, 16 * k, 1), low)
                    x[e + k] = jnp.where(upper, high, pltpu.roll(low, 128 - 16 * k, 1))
        for b in range(6):
            table[h, 8 * b : 8 * b + 8, :] = x[b]


def split(table, left):
    for h in range(8):
        values = table[h]
        hi = values.astype(BF16)
        lo = (values - hi.astype(F32)).astype(BF16)
        at = pl.ds(128 * (h % 2), 128)
        left[96 * (h // 2) : 96 * (h // 2) + 48, at] = hi
        left[96 * (h // 2) + 48 : 96 * (h // 2) + 96, at] = lo


def choose(left, pick_ref, g, upper, store):
    chosen = lax.dot_general(
        left[...], one_hot(pick_ref, g, 0, 0, 16, 15, upper), (((1,), (0,)), ((), ())),
        preferred_element_type=F32,
    )
    for j in range(8):
        quarter = (jnp.broadcast_to(pick_ref[g * 8 + j : g * 8 + j + 1, :], (8, 128)) >> 8) & 3
        low, high = (quarter & 1) == 1, quarter > 1
        at = slice(128 * j, 128 * j + 128)
        for r in range(0, 48, 8):
            y = [chosen[96 * q + r : 96 * q + r + 8, at] + chosen[96 * q + 48 + r : 96 * q + 56 + r, at]
                 for q in range(4)]
            store(j, r, jnp.where(high, jnp.where(low, y[3], y[2]), jnp.where(low, y[1], y[0])))


def last(theirs, pick_ref, red_ref, rows_ref, near_ref, inv_ref, out_ref, left, picked, outs):
    split(theirs, left)
    inv_ref[...] = jnp.transpose(rows_ref[...])[0:16, 0:81]
    for g in range(8):
        base = (g % 2) * (8 * PS)

        def store(j, r, value):
            at = (g * 8 + j) * 48 + r
            picked[base + PS * j + r : base + PS * j + r + 8, :] = value + near_ref[at : at + 8, :]

        choose(left, pick_ref, g, 1, store)
        part = [red_ref[c, g * 8 : g * 8 + 8, :] for c in range(9)]
        total = [None] * 9
        for pos, (i, j) in enumerate(PAIRS):
            value = picked[pl.ds(base + pos, 8, stride=PS), :]
            for r, c in sorted({(i, j), (j, i)}):
                x = value * part[c]
                total[r] = x if total[r] is None else total[r] + x
        base = (g % 2) * (8 * OS)
        for r in range(9):
            outs[pl.ds(base + r, 8, stride=OS), :] = total[r]
        for j in range(8):
            at = pl.ds((g * 8 + j) * 128, 128)
            out_ref[0:8, at] = outs[base + j * OS : base + j * OS + 8, :]
            out_ref[8:9, at] = outs[base + j * OS + 8 : base + j * OS + 9, :]


def kernel(cam_hbm, pt_hbm, res_hbm, pid_hbm, cid_hbm, map_hbm, rank_hbm, theirs, pick_ref, red, rows_ref, near_ref,
           cam_ref, pt_ref, res_ref, pid_ref, cid_ref, map_ref, rank_ref, pos_ref,
           xs, ts, tot, heads, tails, fix, rhs, acc, ent,
           part, swap, half, recv, owned, mine, table, left, load_sems, swap_sems, send_sems, recv_sems):
    pts, core = lax.axis_index("pts"), lax.axis_index("grp")
    partner = (pts, 1 - core)
    chip_z = [(((pts >> 4) + d) & 3) << 4 for d in range(4)]
    chip_x = [(((pts >> 2) + d) & 3) << 2 for d in range(4)]
    chip_y = [(pts + d) & 3 for d in range(4)]

    def chip(off):
        return chip_z[off >> 4] + chip_x[(off >> 2) & 3] + chip_y[off & 3]

    pairs = [(pt_hbm, pt_ref), (res_hbm, res_ref), (pid_hbm, pid_ref), (cid_hbm, cid_ref),
             (map_hbm, map_ref), (rank_hbm, rank_ref), (cam_hbm, cam_ref)]
    loads = [pltpu.make_async_copy(src, dst, load_sems.at[n]) for n, (src, dst) in enumerate(pairs)]
    for load in loads[0:6]:
        load.start()
    barrier = pltpu.get_barrier_semaphore()
    peers = [partner] + [(chip(off), core) for off in OFFSETS[:-1]]
    peers += [(chip(off), 1 - core) for off in OFFSETS[:-1] if off in OFFSETS[CLOSE:] or back(off) in OFFSETS[CLOSE:]]
    for peer in peers:
        pl.semaphore_signal(barrier, inc=1, device_id=peer, device_id_type=MESH)
    loads[6].start()

    with jax.named_scope("load"):
        for load in loads[0:3]:
            load.wait()
        spread_points(pt_ref, res_ref, xs)

    def cameras_in():
        for load in loads[3:]:
            load.wait()
        find_slots(pts, core, cid_ref, map_ref, rank_ref, pos_ref, pick_ref)
        spread_cameras(cam_ref, xs)

    def swap_of(n):
        some = pl.ds(n * EACH, EACH)
        return pltpu.make_async_remote_copy(
            src_ref=part.at[some, 1 - core], dst_ref=swap.at[some], send_sem=swap_sems.at[n],
            recv_sem=swap_sems.at[PARTS + n], device_id=partner, device_id_type=MESH)

    def give(src, slot, device):
        pltpu.make_async_remote_copy(
            src_ref=src, dst_ref=recv.at[slot], send_sem=send_sems.at[0], recv_sem=recv_sems.at[0],
            device_id=device, device_id_type=MESH).start()

    def send(n):
        swap_of(n).wait()
        for r in range(n * EACH, n * EACH + EACH):
            half[r] = part[r, core] + swap[r]
        for r in range(n * EACH, n * EACH + EACH):
            give(half.at[r], r, (chip(OFFSETS[r]), core))

    def done(n):
        with jax.named_scope("send"):
            for r in range(n * EACH, n * EACH + EACH):
                at = pl.ds(r * 16, 16)
                part[r] = (acc[at, 0:128] + acc[at, 128:256]).reshape(2, 8, 128)
            if n == 0:
                pl.semaphore_wait(barrier, len(peers))
            if n < PARTS - 1:
                swap_of(n).start()
            else:
                for r in range(CLOSE, CHIPS):
                    to = chip(OFFSETS[r])
                    if r < CHIPS - 1:
                        give(part.at[r, core], r, (to, core))
                    give(part.at[r, 1 - core], CHIPS - 1 + r - CLOSE, (to, 1 - core))

    with jax.named_scope("points"):
        point_sums(pid_ref, xs, tot, heads, tails, fix, cameras_in)
    with jax.named_scope("cameras"):
        camera_sums(pid_ref, pos_ref, xs, tot, fix, red, ts, rhs, acc, done, send)
    with jax.named_scope("scatter"):
        pltpu.make_async_copy(recv, recv, recv_sems.at[0]).wait()

    with jax.named_scope("invert"):
        sums = [recv[n] for n in range(CHIPS - 1 + EACH)] + [part[CHIPS - 1, core]]
        while len(sums) > 1:
            sums = [sums[i] + sums[i + 1] for i in range(0, len(sums) - 1, 2)] + sums[len(sums) & ~1 :]
        owned[...] = invert(sums[0], ent, rows_ref)
        mine[CHIPS - 1] = owned[...]

    with jax.named_scope("gather"):
        for off in OFFSETS[:-1]:
            pltpu.make_async_remote_copy(
                src_ref=owned, dst_ref=mine.at[RANK[back(off)]], send_sem=send_sems.at[1],
                recv_sem=recv_sems.at[1], device_id=(chip(off), core), device_id_type=MESH).start()
        others = recv.at[0 : CHIPS - 1]
        pltpu.make_async_copy(others, others, recv_sems.at[1]).wait()
    with jax.named_scope("near"):
        across = pltpu.make_async_remote_copy(
            src_ref=table, dst_ref=theirs, send_sem=swap_sems.at[0], recv_sem=swap_sems.at[PARTS],
            device_id=partner, device_id_type=MESH)
        arrange(mine, table)
        split(table, left)
        across.start()
        for g in range(8):
            def store(j, r, value):
                at = (g * 8 + j) * 48 + r
                near_ref[at : at + 8, :] = value

            choose(left, pick_ref, g, 0, store)
    with jax.named_scope("across"):
        pltpu.make_async_copy(recv, recv, send_sems.at[0]).wait()
        pltpu.make_async_copy(others, others, send_sems.at[1]).wait()
        across.wait()


def shards(cam_jac, pt_jac, resid, obs_point, obs_camera, camera_slot):
    vm = pltpu.VMEM
    dma = pltpu.SemaphoreType.DMA
    shape = jax.ShapeDtypeStruct
    ranks = np.zeros((8, 128), np.int32)
    ranks[:, OFFSETS] = np.arange(CHIPS)
    ranks = jnp.asarray(ranks)
    theirs, picks, red, rows, near = pl.pallas_call(
        kernel,
        out_shape=(
            shape((8, 48, 128), F32),
            shape((64, 128), I32),
            shape((9, 64, 128), F32),
            shape((128, 128), F32),
            shape((64 * 48, 128), F32),
        ),
        in_specs=[pl.BlockSpec(memory_space=pltpu.HBM)] * 7,
        out_specs=[pl.BlockSpec(memory_space=vm)] * 5,
        scratch_shapes=[
            vm((18, 8192), F32),
            vm((6, 8192), F32),
            vm((2, 8192), F32),
            vm((64, 128), I32),
            vm((64, 128), I32),
            vm((16, 128), I32),
            vm((8, 128), I32),
            vm((64, 128), I32),
            vm((64 * XS, 128), F32),
            vm((16 * TS, 128), F32),
            vm((9 * 64, 128), F32),
            vm((64, 128), F32),
            vm((64, 128), F32),
            vm((128, 128), F32),
            vm((8, 1024, 256), BF16),
            vm((1024, 256), F32),
            vm((64, 128), F32),
            vm((CHIPS, 2, 8, 128), F32),
            vm((CLOSE, 8, 128), F32),
            vm((CLOSE, 8, 128), F32),
            vm((CHIPS - 1 + EACH, 8, 128), F32),
            vm((8, 128), F32),
            vm((CHIPS, 8, 128), F32),
            vm((8, 48, 128), F32),
            vm((384, 256), BF16),
            dma((7,)),
            dma((2 * PARTS,)),
            dma((2,)),
            dma((6,)),
        ],
        compiler_params=pltpu.CompilerParams(
            vmem_limit_bytes=28 * 2**20, collective_id=0, has_side_effects=True
        ),
        name="schur",
    )(
        *[
            pltpu.with_memory_space_constraint(x, pltpu.HBM)
            for x in (
                cam_jac,
                pt_jac,
                resid,
                obs_point.reshape(64, 128),
                obs_camera.reshape(64, 128),
                camera_slot.reshape(16, 128),
                ranks,
            )
        ]
    )
    inverse, precond = pl.pallas_call(
        last,
        out_shape=(shape((16, 81), F32), shape((9, 8192), F32)),
        in_specs=[pl.BlockSpec(memory_space=vm)] * 5,
        out_specs=[pl.BlockSpec(memory_space=vm)] * 2,
        scratch_shapes=[
            vm((384, 256), BF16),
            vm((16 * PS, 128), F32),
            vm((16 * OS, 128), F32),
        ],
        compiler_params=pltpu.CompilerParams(vmem_limit_bytes=28 * 2**20),
        name="last",
    )(theirs, picks, red, rows, near)
    return inverse.T, precond


def solution(mesh):
    both = ("pts", "grp")
    in_specs = (P(None, both), P(None, both), P(None, both), P(both), P(both), P())
    out_specs = (P(None, both), P(None, both))
    return jax.shard_map(shards, mesh=mesh, in_specs=in_specs, out_specs=out_specs, check_vma=False)
```
